32 devices in a mesh: section: 4 (over z), ctx: 8 (over y, x, core).
Axes of the slice: x: 2, y: 2, z: 4, core: 2. Of those that a mesh axis runs over, the one named last changes fastest.
Arguments:
- queries: bfloat16 [4, 1024, 4096], P('section', 'ctx'), may hold values from -130 to 130
- keys_new: bfloat16 [4, 1024, 1024], P('section', 'ctx'), may hold values from -6 to 6
- values_new: bfloat16 [4, 1024, 1024], P('section', 'ctx'), may hold values from -6 to 6
- stretch_cache: bfloat16 [4, 512, 2048], P('section'), may hold values from -6 to 6
- hadamard_signs: int32 [4, 2, 128], P('section'), may hold values from -1 to 1, as said below
- stretch_docs: int32 [8], replicated, may hold values from 0 to 1, never falling along the last dimension, each value on 1 to 5 neighbouring positions
Outputs:
- handed: bfloat16 [4, 1024, 4096], P('section', 'ctx')
The draws below stay inside these ranges and needn't reach their ends.
Inputs may be any that keep to these rules, and one draw needn't show every extreme that they name: `hadamard_signs`: each entry is -1 or 1. `stretch_docs`: never falling along the stretches; each document covers 1 to 5 stretches in a row.
All inputs are finite; a program needn't handle non-finite values.
Results may differ from the reference program's by a relative error of at most 0.0099.
Values may be sent and summed in bfloat16 or wider, within the bound.
A program may use at most 128 MiB of HBM per device.

```python
import math
import jax
import jax.numpy as jnp
import numpy as np
from jax import lax

QH = 32
KVH = 8
HD = 128
ROWS = 128
CACHE = 256
SECTIONS = 4
STRETCHES = 8
TOKENS = 1024
SPAN = 5
DOCS = 2
N_CTX = 8


def draw_queries(key, part):
    first_key = jax.random.fold_in(jax.random.fold_in(key, 11), 0)
    shape_all = (SECTIONS, TOKENS, QH * HD)
    base = jnp.clip(2.5 * jax.random.normal(first_key, shape_all, jnp.float32), -10.0, 10.0)
    return base.astype(jnp.bfloat16)


def draw_hadamard_signs(key, part):
    picks = jax.random.randint(jax.random.fold_in(key, 23), (SECTIONS, 2, HD), 0, 2)
    return (2 * picks - 1).astype(jnp.int32)


def shard_levels(own_key, extent, cuts, smallest, largest):
    def one(axis_at, shards_of):
        heights = jax.random.uniform(jax.random.fold_in(jax.random.fold_in(own_key, 6), axis_at), (shards_of,), jnp.float32, smallest / len(cuts), largest / len(cuts))
        return jnp.repeat(jnp.exp(heights), extent[axis_at] // shards_of).reshape((-1,) + (1,) * (len(extent) - axis_at - 1))

    gain = one(*cuts[0])
    for cut in cuts[1:]:
        gain = gain * one(*cut)
    return gain


def length_profile(number_of, total, reach, slope):
    loads = [(1 << 20) // math.isqrt(rank ** slope) + 1 for rank in range(2, number_of + 1)]
    surplus, holding = total - reach - (number_of - 1), [1] * (number_of - 1)
    while surplus > 0:
        movable = [i for i in range(number_of - 1) if holding[i] < reach]
        whole, left = sum([loads[i] for i in movable]), surplus
        for i in movable:
            extra = min(reach - holding[i], max(1, left * loads[i] // whole), surplus)
            holding[i] = holding[i] + extra
            surplus = surplus - extra
    return np.array([reach] + holding)


def uneven(key, number_of, total, most, slope):
    if number_of == 2:
        one = jax.random.randint(key, (), max(1, total - most), min(most, total - 1) + 1)
        return jnp.stack([one, total - one])
    tallies = jnp.asarray(length_profile(number_of, total, most, slope), jnp.int32)
    pairs = (number_of - 1) // 2
    donor, sink = tallies[1:1 + 2 * pairs:2], tallies[2:2 + 2 * pairs:2]
    room = jnp.minimum(donor - 1, most - sink)
    passed = jax.random.randint(jax.random.fold_in(key, 1), (pairs,), 0, 1 << 20) % (room + 1)
    tallies = tallies.at[1:1 + 2 * pairs:2].set(donor - passed).at[2:2 + 2 * pairs:2].set(sink + passed)
    return tallies[jax.random.permutation(jax.random.fold_in(key, 2), number_of)]


def centred(rng, extent, width, reach, cuts=(), kind=jnp.bfloat16):
    values = width * jax.random.normal(rng, extent, jnp.float32)
    if cuts:
        values = values * shard_levels(rng, extent, cuts, -0.22, 0.18)
    return jnp.clip(values, -reach, reach).astype(kind)


def setup_inputs(seed: int = 0) -> dict:
    arg_keys = jax.random.split(jax.random.key(seed), 7)
    return {
        "queries": draw_queries(jax.random.fold_in(arg_keys[6], 71), 0),
        "keys_new": centred(arg_keys[1], (SECTIONS, TOKENS, KVH * HD), 1.0, 6.0, ((0, 4), (1, 8))),
        "values_new": centred(arg_keys[2], (SECTIONS, TOKENS, KVH * HD), 1.0, 6.0, ((0, 4), (1, 8))),
        "stretch_cache": centred(arg_keys[3], (SECTIONS, DOCS * CACHE, 2 * KVH * HD), 1.0, 6.0, ((0, 4),)),
        "hadamard_signs": draw_hadamard_signs(jax.random.fold_in(arg_keys[6], 71), 0),
        "stretch_docs": jnp.searchsorted(jnp.cumsum(uneven(arg_keys[5], DOCS, STRETCHES, SPAN, 0)), jnp.arange(STRETCHES), side="right").astype(jnp.int32),
    }


def hadamard(length):
    numbers = np.arange(length)
    common = numbers[:, None] & numbers[None, :]
    parity = np.zeros((length, length), np.int64)
    for bit_place in range(max(int(length).bit_length(), 1)):
        parity = parity ^ ((common >> bit_place) & 1)
    return 1.0 - 2.0 * parity


def rotate(source, sign_row, rotation):
    row_count = source.shape[0]
    head_size = rotation.shape[0]
    shaped = (source.reshape(row_count, -1, head_size) * sign_row.astype(source.dtype)).reshape(-1, head_size)
    turned = jnp.dot(shaped, rotation, preferred_element_type=jnp.float32) * (head_size ** -0.5)
    return turned.reshape(row_count, -1).astype(jnp.bfloat16)


def reference(queries, keys_new, values_new, stretch_cache, hadamard_signs, stretch_docs):
    rotation = jnp.asarray(hadamard(HD), dtype=jnp.bfloat16)
    inverse = jnp.asarray(hadamard(HD), dtype=jnp.float32)
    groups = QH // KVH

    def one_section(section_args):
        section_query, section_keys, section_values, section_cache, section_signs = section_args
        fronts = jnp.concatenate([rotate(section_keys, section_signs[0], rotation), rotate(section_values, section_signs[1], rotation)], axis=1)

        def one_stretch(stretch_index):
            query_rows = lax.dynamic_slice_in_dim(section_query, stretch_index * ROWS, ROWS, 0)
            query_turned = rotate(query_rows, section_signs[0], rotation).reshape(ROWS, KVH, groups, HD)
            doc_mine = stretch_docs[stretch_index]
            own_cache = lax.dynamic_slice_in_dim(section_cache, (doc_mine * CACHE).astype(jnp.int32), CACHE, 0)
            keyset = jnp.concatenate([own_cache, fronts], axis=0)
            key_part = keyset[:, :KVH * HD].reshape(-1, KVH, HD)
            value_part = keyset[:, KVH * HD:].reshape(-1, KVH, HD)
            scores = jnp.einsum("rkgd,nkd->rkgn", query_turned.astype(jnp.float32), key_part.astype(jnp.float32)) * (HD ** -0.5)
            position = jnp.arange(TOKENS, dtype=jnp.int32)
            key_stretch = position // ROWS
            key_row = position % ROWS
            query_row = jnp.arange(ROWS, dtype=jnp.int32)
            doc_keys = stretch_docs[key_stretch]
            same_stretch = (key_stretch[None, :] == stretch_index) & (key_row[None, :] <= query_row[:, None])
            earlier = (key_stretch[None, :] < stretch_index) & (doc_keys[None, :] == doc_mine)
            allowed = jnp.concatenate([jnp.ones((ROWS, CACHE), dtype=bool), same_stretch | earlier], axis=1)
            scores = jnp.where(allowed[:, None, None, :], scores, -jnp.inf)
            row_max = scores.max(-1, keepdims=True)
            exponent = jnp.exp(scores - row_max)
            row_sum = exponent.sum(-1)
            weights = exponent.astype(jnp.bfloat16)
            averaged = jnp.einsum("rkgn,nkd->rkgd", weights.astype(jnp.float32), value_part.astype(jnp.float32)) / row_sum[..., None]
            restored = jnp.dot(averaged.reshape(-1, HD), inverse, precision=lax.Precision.HIGHEST)
            restored = restored * (HD ** -0.5) * section_signs[1].astype(jnp.float32)
            return restored.reshape(ROWS, QH * HD).astype(jnp.bfloat16)

        return lax.map(one_stretch, jnp.arange(N_CTX, dtype=jnp.int32)).reshape(TOKENS, QH * HD)

    heads_out = lax.map(one_section, (queries, keys_new, values_new, stretch_cache, hadamard_signs))
    return jnp.roll(heads_out, 1, axis=0)
```

```python
import functools

import jax
import jax.numpy as jnp
import numpy as np
from jax import lax
from jax.experimental import pallas as pl
from jax.experimental.pallas import tpu as pltpu
from jax.sharding import PartitionSpec as P

CACHE = 256
MESH = pl.DeviceIdType.MESH


def attention_kernel(
    n,
    sections,
    docs_hbm,
    signs_hbm,
    q_hbm,
    k_hbm,
    v_hbm,
    cache_hbm,
    out_ref,
    docs_ref,
    signs_ref,
    q_buf,
    q_send,
    cache_buf,
    own,
    held,
    out_buf,
    small_sem,
    cache_sem,
    q_sem,
    swap_send,
    swap_recv,
    own_sem,
    mine_sem,
    send_sem,
    recv_sem,
    out_send,
    out_recv,
    first_send,
    first_recv,
):
    section = lax.axis_index("section")
    me = lax.axis_index("ctx")
    p = lax.rem(me, 2)
    chip = me // 2
    chips = n // 2
    heads, hd = held.shape[0], held.shape[4]
    rows = held.shape[3]
    slots = held.shape[2]
    back = (slots - 2) // 2
    width = out_buf.shape[3]
    groups = width // hd
    all_heads = 2 * heads
    kv_width = all_heads * hd
    detour = chips == 4
    sibling = me + 1 - 2 * p
    following = lax.rem(section + 1, sections)
    previous = lax.rem(section + sections - 1, sections)

    def cols(start, size):
        return pl.ds(pl.multiple_of(start, hd), size)

    barrier = pltpu.get_barrier_semaphore()

    def greet(sec, ctx):
        pl.semaphore_signal(barrier, inc=1, device_id=(sec, ctx), device_id_type=MESH)

    for d in range(back, 0, -1):
        @pl.when(chip >= d)
        def _(d=d):
            greet(section, 2 * (chip - d))
            greet(section, 2 * (chip - d) + 1)
    greet(previous, 2 * chip)
    greet(previous, 2 * chip + 1)
    greet(section, sibling)

    def own_copies(h):
        return (
            pltpu.make_async_copy(k_hbm.at[:, cols(h * hd, hd)], own.at[h, 0], own_sem.at[h, 0]),
            pltpu.make_async_copy(v_hbm.at[:, cols(h * hd, hd)], own.at[h, 1], own_sem.at[h, 1]),
        )

    def mine_copies(i):
        h = p * heads + i
        slot = slots - 2 + p
        return (
            pltpu.make_async_copy(
                k_hbm.at[:, cols(h * hd, hd)], held.at[i, 0, slot], mine_sem.at[i, 0]
            ),
            pltpu.make_async_copy(
                v_hbm.at[:, cols(h * hd, hd)], held.at[i, 1, slot], mine_sem.at[i, 1]
            ),
        )

    def q_copies(i):
        theirs = (1 - p) * heads + i
        ours = p * heads + i
        return (
            pltpu.make_async_copy(
                q_hbm.at[:, cols(theirs * width, width)], q_send.at[i], q_sem.at[i, 0]
            ),
            pltpu.make_async_copy(
                q_hbm.at[:, cols(ours * width, width)], q_buf.at[p, i], q_sem.at[i, 1]
            ),
        )

    def cache_copies(i):
        h = p * heads + i
        return (
            pltpu.make_async_copy(
                cache_hbm.at[:, cols(h * hd, hd)], cache_buf.at[i, 0], cache_sem.at[i, 0]
            ),
            pltpu.make_async_copy(
                cache_hbm.at[:, cols(kv_width + h * hd, hd)], cache_buf.at[i, 1], cache_sem.at[i, 1]
            ),
        )

    def start_own(i, carry):
        for copy in own_copies(i) + own_copies(heads + i):
            copy.start()
        return carry

    def start_loads(i, carry):
        for copy in mine_copies(i) + cache_copies(i) + q_copies(i):
            copy.start()
        return carry

    small = (
        pltpu.make_async_copy(docs_hbm, docs_ref, small_sem.at[0]),
        pltpu.make_async_copy(signs_hbm, signs_ref, small_sem.at[1]),
    )
    start_own(0, 0)
    for copy in small:
        copy.start()
    start_loads(0, 0)
    lax.fori_loop(1, heads, start_own, 0)
    lax.fori_loop(1, heads, start_loads, 0)

    for d in range(1, back + 1):
        @pl.when(chip < d)
        def _(d=d):
            for i in range(heads):
                at = slots - 2 - 2 * d
                held[i, :, at : at + 2] = jnp.zeros((2, 2, rows, hd), held.dtype)

    low = lax.broadcasted_iota(jnp.int32, (hd, hd), 0) & lax.broadcasted_iota(
        jnp.int32, (hd, hd), 1
    )
    shift = 1
    while 2 * shift < hd:
        shift *= 2
    while shift:
        low = low ^ (low >> shift)
        shift //= 2
    hada = (1 - 2 * (low & 1)).astype(jnp.float32).astype(jnp.bfloat16)

    count = jnp.int32(3)
    for d in range(1, back + 1):
        count = count + jnp.where(chip + d < chips, 2, 0)
    pl.semaphore_wait(barrier, count)

    def remote(src, i, kind, slot, index, target):
        return pltpu.make_async_remote_copy(
            src_ref=src,
            dst_ref=held.at[i, kind, slot],
            send_sem=send_sem.at[index, i, kind],
            recv_sem=recv_sem.at[i, kind, slot],
            device_id=(section, target),
            device_id_type=MESH,
        )

    def swap_q(i):
        return pltpu.make_async_remote_copy(
            src_ref=q_send.at[i],
            dst_ref=q_buf.at[p, i],
            send_sem=swap_send.at[i],
            recv_sem=swap_recv.at[i],
            device_id=(section, sibling),
            device_id_type=MESH,
        )

    def start_swap_q(i):
        q_copies(i)[0].wait()
        swap_q(i).start()

    def swap_kv(i, kind):
        return remote(own.at[(1 - p) * heads + i, kind], i, kind, slots - 2 + p, 0, sibling)

    def ahead(i, act):
        for core in range(2):
            for kind in range(2):
                for d in range(1, back + 1):
                    go = chip + d < chips
                    if detour and d == 1:
                        go = go & (chip != 1)

                    @pl.when(go)
                    def _(core=core, kind=kind, d=d):
                        act(
                            remote(
                                own.at[core * heads + i, kind],
                                i,
                                kind,
                                slots - 2 - 2 * d + p,
                                2 * d - 1 + core,
                                2 * (chip + d) + core,
                            )
                        )

    def relays(i, act):
        if detour:
            @pl.when(chip == chips - 1)
            def _():
                for kind in range(2):
                    for slot in range(2):
                        act(
                            remote(
                                held.at[i, kind, slot], i, kind, slot + 2, 1 + slot, me - 2
                            ),
                            kind,
                            slot,
                        )

    def relay(i):
        def act(copy, kind, slot):
            arrived(i, kind, slot)
            copy.start()

        relays(i, act)

    def arrived(i, kind, slot):
        remote(own.at[0, kind], i, kind, slot, 0, sibling).wait_recv()

    def earlier(i, kind, slot):
        there = chip - back + slot // 2 >= 0
        if detour and slot < 2:
            there = there & (chip != chips - 1)

        @pl.when(there)
        def _():
            arrived(i, kind, slot)

    def send(i, carry):
        for copy in own_copies(i) + own_copies(heads + i):
            copy.wait()
        ahead(i, lambda copy: copy.start())
        for kind in range(2):
            swap_kv(i, kind).start()
        return carry

    lax.fori_loop(0, heads, send, 0)
    start_swap_q(0)

    for copy in small:
        copy.wait()
    root = hd ** -0.5
    sign_k = signs_ref[0:1, :].astype(jnp.float32) * root
    sign_v = signs_ref[1:2, :].astype(jnp.float32) * root
    factor = root * float(np.log2(np.e))
    causal = lax.broadcasted_iota(jnp.int32, (rows, rows), 1) <= lax.broadcasted_iota(
        jnp.int32, (rows, rows), 0
    )

    def out_copy(i, e):
        return pltpu.make_async_remote_copy(
            src_ref=out_buf.at[i, e],
            dst_ref=out_ref.at[:, cols((p * heads + i) * width, width)],
            send_sem=out_send.at[i, e],
            recv_sem=out_recv.at[p * heads + i],
            device_id=(following, 2 * chip + e),
            device_id_type=MESH,
        )

    def first_copy(g):
        return pltpu.make_async_remote_copy(
            src_ref=out_buf.at[0, p, :, g * hd : (g + 1) * hd],
            dst_ref=out_ref.at[:, cols(p * heads * width + g * hd, hd)],
            send_sem=first_send.at[g],
            recv_sem=first_recv.at[g],
            device_id=(following, me),
            device_id_type=MESH,
        )

    def step(t, carry):
        i = t // 2
        half = lax.rem(t, 2)
        e = (p + half) - 2 * p * half

        @pl.when(half == 0)
        def _():
            for copy in cache_copies(i):
                copy.wait()

            @pl.when(i + 1 < heads)
            def _():
                start_swap_q(i + 1)

        stretch = 2 * chip + e
        doc = docs_ref[stretch]
        picks = [
            jnp.full((1, hd), jnp.where(doc == k, 1.0, 0.0), jnp.float32).astype(jnp.bfloat16)
            for k in range(cache_buf.shape[2] // CACHE)
        ]

        def cache_block(kind):
            terms = [
                cache_buf[i, kind, k * CACHE : (k + 1) * CACHE, :] * pick
                for k, pick in enumerate(picks)
            ]
            return functools.reduce(jnp.add, terms)

        back_k = jnp.dot(cache_block(0), hada, preferred_element_type=jnp.float32)
        back_v = jnp.dot(cache_block(1), hada, preferred_element_type=jnp.float32)
        back_k = (back_k * sign_k).astype(jnp.bfloat16)
        back_v = (back_v * sign_v).astype(jnp.bfloat16)
        biases = []
        for d in range(slots - 2, 0, -1):
            seen = (stretch >= d) & (docs_ref[jnp.maximum(stretch - d, 0)] == doc)
            biases.append(jnp.where(seen, 0.0, -jnp.inf).astype(jnp.float32))

        def waits(kind):
            sibling_slot = slots - 1 - p
            first = half == 0

            @pl.when(first)
            def _():
                mine_copies(i)[kind].wait()
                for slot in range(1, slots - 2):
                    earlier(i, kind, slot)

            @pl.when(e == 0)
            def _():
                earlier(i, kind, 0)

            @pl.when(e == 1)
            def _():
                arrived(i, kind, sibling_slot)

        @pl.when(half == 0)
        def _():
            q_copies(i)[1].wait()

        @pl.when(half == 1)
        def _():
            swap_q(i).wait_recv()

        waits(0)
        waits(1)
        span = (slots - 1) * rows
        keys = held[i, 0, pl.ds(e, slots - 1)].reshape(span, hd)
        values = held[i, 1, pl.ds(e, slots - 1)].reshape(span, hd)
        keys = jnp.concatenate([back_k, keys], axis=0)
        values = jnp.concatenate([back_v, values], axis=0)
        for g in range(groups):
            query = q_buf[e, i, :, g * hd : (g + 1) * hd]
            scores = lax.dot_general(
                query, keys, (((1,), (1,)), ((), ())), preferred_element_type=jnp.float32
            )
            parts = [scores[:, at : at + rows] for at in range(0, CACHE, rows)]
            for d in range(slots - 2):
                at = CACHE + rows * d
                parts.append(scores[:, at : at + rows] + biases[d])
            parts.append(jnp.where(causal, scores[:, CACHE + span - rows :], -jnp.inf))
            top = functools.reduce(jnp.maximum, parts)
            top = jnp.max(top, axis=1, keepdims=True)
            expo = [jnp.exp2((part - top) * factor) for part in parts]
            total = jnp.sum(functools.reduce(jnp.add, expo), axis=1, keepdims=True)
            weights = jnp.concatenate([part.astype(jnp.bfloat16) for part in expo], axis=1)
            summed = jnp.dot(weights, values, preferred_element_type=jnp.float32)
            out_buf[i, e, :, g * hd : (g + 1) * hd] = (summed / total).astype(out_buf.dtype)

            @pl.when(t == 0)
            def _(g=g):
                first_copy(g).start()

        @pl.when(t > 0)
        def _():
            out_copy(i, e).start()

        @pl.when((half == 1) & (i + 1 < heads))
        def _():
            relay(i + 1)

        return carry

    relay(0)
    lax.fori_loop(0, 2 * heads, step, 0)

    def finish(i, carry):
        ahead(i, lambda copy: copy.wait_send())
        relays(i, lambda copy, kind, slot: copy.wait_send())
        for kind in range(2):
            swap_kv(i, kind).wait_send()
        swap_q(i).wait_send()
        return carry

    lax.fori_loop(0, heads, finish, 0)
    for g in range(groups):
        first_copy(g).wait_send()

    def sent(t, carry):
        half = lax.rem(t, 2)
        out_copy(t // 2, (p + half) - 2 * p * half).wait_send()
        return carry

    lax.fori_loop(1, 2 * heads, sent, 0)

    def received(core, i):
        return pltpu.make_async_remote_copy(
            src_ref=out_buf.at[i, 0],
            dst_ref=out_ref.at[:, cols((core * heads + i) * width, width)],
            send_sem=out_send.at[i, 0],
            recv_sem=out_recv.at[core * heads + i],
            device_id=(following, me),
            device_id_type=MESH,
        )

    for g in range(groups):
        first_copy(g).wait_recv()
    received(1 - p, 0).wait_recv()
    for i in range(1, heads):
        for core in range(2):
            received(core, i).wait_recv()


def per_device(n, sections, queries, keys_new, values_new, stretch_cache, signs, docs):
    rows, q_width = queries.shape[1:]
    kv_width = keys_new.shape[-1]
    hd = signs.shape[-1]
    all_heads = kv_width // hd
    heads = all_heads // 2
    width = q_width // all_heads
    groups = width // hd
    reach = n // 2
    slots = reach + 2
    cached = stretch_cache.shape[1]
    dtype = queries.dtype
    dma = pltpu.SemaphoreType.DMA
    in_hbm = pl.BlockSpec(memory_space=pltpu.HBM)
    out = pl.pallas_call(
        functools.partial(attention_kernel, n, sections),
        out_shape=pltpu.VMEM((rows, q_width), dtype),
        in_specs=[in_hbm] * 6,
        out_specs=pl.BlockSpec(memory_space=pltpu.VMEM),
        scratch_shapes=[
            pltpu.SMEM(docs.shape, docs.dtype),
            pltpu.VMEM(signs.shape[1:], signs.dtype),
            pltpu.VMEM((2, heads, rows, width), dtype),
            pltpu.VMEM((heads, rows, width), dtype),
            pltpu.VMEM((heads, 2, cached, hd), dtype),
            pltpu.VMEM((all_heads, 2, rows, hd), dtype),
            pltpu.VMEM((heads, 2, slots, rows, hd), dtype),
            pltpu.VMEM((heads, 2, rows, width), dtype),
            dma((2,)),
            dma((heads, 2)),
            dma((heads, 2)),
            dma((heads,)),
            dma((heads,)),
            dma((all_heads, 2)),
            dma((heads, 2)),
            dma((reach + 1, heads, 2)),
            dma((heads, 2, slots)),
            dma((heads, 2)),
            dma((all_heads,)),
            dma((groups,)),
            dma((groups,)),
        ],
        compiler_params=pltpu.CompilerParams(
            collective_id=0, has_side_effects=True, vmem_limit_bytes=58 * 1024 * 1024
        ),
    )(docs, signs[0], queries[0], keys_new[0], values_new[0], stretch_cache[0])
    return out[None]


def solution(mesh):
    in_specs = (
        P("section", "ctx", None),
        P("section", "ctx", None),
        P("section", "ctx", None),
        P("section", None, None),
        P("section", None, None),
        P(),
    )
    out_specs = P("section", "ctx", None)
    body = functools.partial(per_device, mesh.shape["ctx"], mesh.shape["section"])
    return jax.shard_map(body, mesh=mesh, in_specs=in_specs, out_specs=out_specs, check_vma=False)
```

```python
import functools

import jax
import jax.numpy as jnp
import numpy as np
from jax import lax
from jax.experimental import pallas as pl
from jax.experimental.pallas import tpu as pltpu
from jax.sharding import PartitionSpec as P

CACHE = 256
MESH = pl.DeviceIdType.MESH


def attention_kernel(
    n,
    sections,
    docs_hbm,
    signs_hbm,
    q_hbm,
    k_hbm,
    v_hbm,
    cache_hbm,
    out_ref,
    docs_ref,
    signs_ref,
    q_buf,
    q_send,
    cache_buf,
    own,
    held,
    out_buf,
    small_sem,
    cache_sem,
    q_sem,
    swap_send,
    swap_recv,
    own_sem,
    mine_sem,
    send_sem,
    recv_sem,
    out_send,
    out_recv,
):
    section = lax.axis_index("section")
    me = lax.axis_index("ctx")
    p = lax.rem(me, 2)
    chip = me // 2
    chips = n // 2
    heads, hd = held.shape[0], held.shape[4]
    rows = held.shape[3]
    slots = held.shape[2]
    back = (slots - 2) // 2
    width = out_buf.shape[3]
    groups = width // hd
    all_heads = 2 * heads
    kv_width = all_heads * hd
    detour = chips == 4
    sibling = me + 1 - 2 * p
    following = lax.rem(section + 1, sections)
    previous = lax.rem(section + sections - 1, sections)

    def cols(start, size):
        return pl.ds(pl.multiple_of(start, hd), size)

    barrier = pltpu.get_barrier_semaphore()

    def greet(sec, ctx):
        pl.semaphore_signal(barrier, inc=1, device_id=(sec, ctx), device_id_type=MESH)

    own_copies = (
        pltpu.make_async_copy(k_hbm, own.at[0], own_sem),
        pltpu.make_async_copy(v_hbm, own.at[1], own_sem),
    )

    def mine_copies(i):
        at = cols((p * heads + i) * hd, hd)
        slot = slots - 2 + p
        return (
            pltpu.make_async_copy(k_hbm.at[:, at], held.at[i, 0, slot], mine_sem),
            pltpu.make_async_copy(v_hbm.at[:, at], held.at[i, 1, slot], mine_sem),
        )

    span = heads * width
    q_copies = (
        pltpu.make_async_copy(q_hbm.at[:, cols(p * span, span)], q_buf.at[p], q_sem.at[0]),
        pltpu.make_async_copy(q_hbm.at[:, cols((1 - p) * span, span)], q_send, q_sem.at[1]),
    )
    reach = heads * hd
    cache_copies = (
        pltpu.make_async_copy(
            cache_hbm.at[:, cols(p * reach, reach)], cache_buf.at[0], cache_sem
        ),
        pltpu.make_async_copy(
            cache_hbm.at[:, cols(kv_width + p * reach, reach)], cache_buf.at[1], cache_sem
        ),
    )
    small = (
        pltpu.make_async_copy(docs_hbm, docs_ref, small_sem.at[0]),
        pltpu.make_async_copy(signs_hbm, signs_ref, small_sem.at[1]),
    )
    def all_of(ref, sem):
        return pltpu.make_async_remote_copy(
            src_ref=ref,
            dst_ref=ref,
            send_sem=sem,
            recv_sem=sem,
            device_id=(section, sibling),
            device_id_type=MESH,
        )

    for copy in own_copies:
        copy.start()

    for d in range(back, 0, -1):
        come = chip >= d
        if detour and d == 1:
            come = come & ((chip != 2) | (p == 0))

        @pl.when(come)
        def _(d=d):
            greet(section, 2 * (chip - d))
            greet(section, 2 * (chip - d) + 1)
    if detour:
        @pl.when(chip == 2)
        def _():
            greet(section, me + 2)
    greet(section, sibling)
    greet(previous, 2 * chip)
    greet(previous, 2 * chip + 1)

    for copy in small + mine_copies(0) + cache_copies + q_copies:
        copy.start()
    for i in range(1, heads):
        for copy in mine_copies(i):
            copy.start()

    for d in range(1, back + 1):
        @pl.when(chip < d)
        def _(d=d):
            for i in range(heads):
                at = slots - 2 - 2 * d
                held[i, :, at : at + 2] = jnp.zeros((2, 2, rows, hd), held.dtype)

    low = lax.broadcasted_iota(jnp.int32, (hd, hd), 0) & lax.broadcasted_iota(
        jnp.int32, (hd, hd), 1
    )
    shift = 1
    while 2 * shift < hd:
        shift *= 2
    while shift:
        low = low ^ (low >> shift)
        shift //= 2
    hada = (1 - 2 * (low & 1)).astype(jnp.float32).astype(jnp.bfloat16)

    count = jnp.int32(3)
    for d in range(1, back + 1):
        count = count + jnp.where(chip + d < chips, 2, 0)
    if detour:
        count = count + jnp.where(chip == chips - 1, 1, 0) - jnp.where(chip == 1, 1, 0)
    pl.semaphore_wait(barrier, count)

    def remote(src, dst, index, i, pair, target):
        return pltpu.make_async_remote_copy(
            src_ref=src,
            dst_ref=dst,
            send_sem=send_sem.at[index],
            recv_sem=recv_sem.at[i, pair],
            device_id=(section, target),
            device_id_type=MESH,
        )

    swap_q = pltpu.make_async_remote_copy(
        src_ref=q_send,
        dst_ref=q_buf.at[p],
        send_sem=swap_send,
        recv_sem=swap_recv,
        device_id=(section, sibling),
        device_id_type=MESH,
    )

    def piece(h):
        return own.at[:, :, cols(h * hd, hd)]

    def swap_kv(i):
        block = piece((1 - p) * heads + i)
        return remote(block, held.at[i, :, slots - 2 + p], 0, i, back, sibling)

    def ahead(i):
        for core in range(2):
            for d in range(1, back + 1):
                go = chip + d < chips
                if detour and d == 1:
                    go = go & ((chip != 1) | (i == 0)) if core == 0 else go & (chip != 1)

                @pl.when(go)
                def _(core=core, d=d):
                    slot = slots - 2 - 2 * d + p
                    block = piece(core * heads + i)
                    target = 2 * (chip + d) + core
                    remote(
                        block, held.at[i, :, slot], 2 * d - 1 + core, i, back - d, target
                    ).start()

    def relay_copy(i):
        return remote(held.at[i, :, 0:2], held.at[i, :, 2:4], 1, i, 1, me - 2)

    def arrived(i, pair):
        block = held.at[i, :, 2 * pair : 2 * pair + 2]
        remote(block, block, 0, i, pair, sibling).wait_recv()

    relays = (chip == chips - 1) if detour else False

    def relay(i):
        if detour:
            @pl.when(relays)
            def _():
                arrived(i, 0)

                @pl.when((i > 0) | (p == 1))
                def _():
                    relay_copy(i).start()

    def send(i, carry):
        swap_kv(i).start()
        ahead(i)
        return carry

    all_of(own, own_sem).wait_recv()
    lax.fori_loop(0, heads, send, 0)
    q_copies[1].wait()
    swap_q.start()

    for copy in small:
        copy.wait()
    root = hd ** -0.5
    sign_k = signs_ref[0:1, :].astype(jnp.float32) * root
    sign_v = signs_ref[1:2, :].astype(jnp.float32) * root
    factor = root * float(np.log2(np.e))
    causal = lax.broadcasted_iota(jnp.int32, (rows, rows), 1) <= lax.broadcasted_iota(
        jnp.int32, (rows, rows), 0
    )

    def out_copy(i, e):
        return pltpu.make_async_remote_copy(
            src_ref=out_buf.at[i, e],
            dst_ref=out_ref.at[:, cols((p * heads + i) * width, width)],
            send_sem=out_send,
            recv_sem=out_recv,
            device_id=(following, 2 * chip + e),
            device_id_type=MESH,
        )

    def first_copy(g):
        return pltpu.make_async_remote_copy(
            src_ref=out_buf.at[0, p, :, g * hd : (g + 1) * hd],
            dst_ref=out_ref.at[:, cols(p * heads * width + g * hd, hd)],
            send_sem=out_send,
            recv_sem=out_recv,
            device_id=(following, me),
            device_id_type=MESH,
        )

    def step(t, carry):
        i = t // 2
        half = lax.rem(t, 2)
        e = (p + half) - 2 * p * half

        @pl.when(t == 0)
        def _():
            all_of(cache_buf, cache_sem).wait_recv()
            all_of(held.at[:, :, slots - 2 + p], mine_sem).wait_recv()
            q_copies[0].wait()

        stretch = 2 * chip + e
        doc = docs_ref[stretch]
        picks = [
            jnp.full((1, hd), jnp.where(doc == k, 1.0, 0.0), jnp.float32).astype(jnp.bfloat16)
            for k in range(cache_buf.shape[1] // CACHE)
        ]

        def cache_block(kind):
            terms = [
                cache_buf[kind, k * CACHE : (k + 1) * CACHE, cols(i * hd, hd)] * pick
                for k, pick in enumerate(picks)
            ]
            return functools.reduce(jnp.add, terms)

        back_k = jnp.dot(cache_block(0), hada, preferred_element_type=jnp.float32)
        back_v = jnp.dot(cache_block(1), hada, preferred_element_type=jnp.float32)
        back_k = (back_k * sign_k).astype(jnp.bfloat16)
        back_v = (back_v * sign_v).astype(jnp.bfloat16)
        biases = []
        for d in range(slots - 2, 0, -1):
            seen = (stretch >= d) & (docs_ref[jnp.maximum(stretch - d, 0)] == doc)
            biases.append(jnp.where(seen, 0.0, -jnp.inf).astype(jnp.float32))

        @pl.when(half == 0)
        def _():
            for pair in range(back):
                there = chip - back + pair >= 0
                if detour and pair == 0:
                    there = there & (chip != chips - 1)

                @pl.when(there)
                def _(pair=pair):
                    arrived(i, pair)

        @pl.when(half == 1 - p)
        def _():
            block = held.at[i, :, slots - 1 - p]
            remote(block, block, 0, i, back, sibling).wait_recv()

        @pl.when(t == 1)
        def _():
            swap_q.wait_recv()

        span_new = (slots - 1) * rows
        keys = held[i, 0, pl.ds(e, slots - 1)].reshape(span_new, hd)
        values = held[i, 1, pl.ds(e, slots - 1)].reshape(span_new, hd)
        keys = jnp.concatenate([back_k, keys], axis=0)
        values = jnp.concatenate([back_v, values], axis=0)
        for g in range(groups):
            query = q_buf[e, :, cols(i * width + g * hd, hd)]
            scores = lax.dot_general(
                query, keys, (((1,), (1,)), ((), ())), preferred_element_type=jnp.float32
            )
            parts = [scores[:, at : at + rows] for at in range(0, CACHE, rows)]
            for d in range(slots - 2):
                at = CACHE + rows * d
                parts.append(scores[:, at : at + rows] + biases[d])
            parts.append(jnp.where(causal, scores[:, CACHE + span_new - rows :], -jnp.inf))
            top = functools.reduce(jnp.maximum, parts)
            top = jnp.max(top, axis=1, keepdims=True)
            expo = [jnp.exp2((part - top) * factor) for part in parts]
            total = jnp.sum(functools.reduce(jnp.add, expo), axis=1, keepdims=True)
            weights = jnp.concatenate([part.astype(jnp.bfloat16) for part in expo], axis=1)
            summed = jnp.dot(weights, values, preferred_element_type=jnp.float32)
            out_buf[i, e, :, g * hd : (g + 1) * hd] = (summed / total).astype(out_buf.dtype)

            @pl.when(t == 0)
            def _(g=g):
                first_copy(g).start()

        @pl.when(t > 0)
        def _():
            out_copy(i, e).start()

        @pl.when((half == 0) & (i + 1 < heads))
        def _():
            relay(i + 1)

        return carry

    relay(0)
    lax.fori_loop(0, 2 * heads, step, 0)

    def leaving(core):
        return own.at[:, :, cols(core * heads * hd, heads * hd)]

    all_of(leaving(1 - p), send_sem.at[0]).wait_send()
    swap_q.wait_send()
    for core in range(2):
        for d in range(1, back + 1):
            go = chip + d < chips
            if detour and d == 1:
                go = go & (chip != 1)

            @pl.when(go)
            def _(core=core, d=d):
                all_of(leaving(core), send_sem.at[2 * d - 1 + core]).wait_send()
    if detour:
        @pl.when(chip == 1)
        def _():
            all_of(piece(0), send_sem.at[1]).wait_send()

        @pl.when(relays & (p == 0))
        def _():
            all_of(held.at[1:, :, 0:2], send_sem.at[1]).wait_send()

        @pl.when(relays & (p == 1))
        def _():
            all_of(held.at[:, :, 0:2], send_sem.at[1]).wait_send()
    all_of(out_buf, out_send).wait_send()
    all_of(out_ref, out_recv).wait_recv()


def per_device(n, sections, queries, keys_new, values_new, stretch_cache, signs, docs):
    rows, q_width = queries.shape[1:]
    kv_width = keys_new.shape[-1]
    hd = signs.shape[-1]
    all_heads = kv_width // hd
    heads = all_heads // 2
    width = q_width // all_heads
    groups = width // hd
    reach = n // 2
    slots = reach + 2
    cached = stretch_cache.shape[1]
    dtype = queries.dtype
    dma = pltpu.SemaphoreType.DMA
    in_hbm = pl.BlockSpec(memory_space=pltpu.HBM)
    out = pl.pallas_call(
        functools.partial(attention_kernel, n, sections),
        out_shape=pltpu.VMEM((rows, q_width), dtype),
        in_specs=[in_hbm] * 6,
        out_specs=pl.BlockSpec(memory_space=pltpu.VMEM),
        scratch_shapes=[
            pltpu.SMEM(docs.shape, docs.dtype),
            pltpu.VMEM(signs.shape[1:], signs.dtype),
            pltpu.VMEM((2, rows, heads * width), dtype),
            pltpu.VMEM((rows, heads * width), dtype),
            pltpu.VMEM((2, cached, heads * hd), dtype),
            pltpu.VMEM((2, rows, kv_width), dtype),
            pltpu.VMEM((heads, 2, slots, rows, hd), dtype),
            pltpu.VMEM((heads, 2, rows, width), dtype),
            dma((2,)),
            dma,
            dma((2,)),
            dma,
            dma,
            dma,
            dma,
            dma((reach + 1,)),
            dma((heads, reach // 2 + 1)),
            dma,
            dma,
        ],
        compiler_params=pltpu.CompilerParams(
            collective_id=0, has_side_effects=True, vmem_limit_bytes=58 * 1024 * 1024
        ),
    )(docs, signs[0], queries[0], keys_new[0], values_new[0], stretch_cache[0])
    return out[None]


def solution(mesh):
    in_specs = (
        P("section", "ctx", None),
        P("section", "ctx", None),
        P("section", "ctx", None),
        P("section", None, None),
        P("section", None, None),
        P(),
    )
    out_specs = P("section", "ctx", None)
    body = functools.partial(per_device, mesh.shape["ctx"], mesh.shape["section"])
    return jax.shard_map(body, mesh=mesh, in_specs=in_specs, out_specs=out_specs, check_vma=False)
```

```python
import functools

import jax
import jax.numpy as jnp
import numpy as np
from jax import lax
from jax.experimental import pallas as pl
from jax.experimental.pallas import tpu as pltpu
from jax.sharding import PartitionSpec as P

CACHE = 256
LENT = (3, 7)
MESH = pl.DeviceIdType.MESH


def attention_kernel(
    n,
    sections,
    docs_hbm,
    signs_hbm,
    q_hbm,
    k_hbm,
    v_hbm,
    cache_hbm,
    out_ref,
    docs_ref,
    signs_ref,
    q_buf,
    q_send,
    cache_buf,
    own,
    held,
    out_buf,
    small_sem,
    cache_sem,
    q_sem,
    swap_send,
    swap_recv,
    own_sem,
    mine_sem,
    send_sem,
    recv_sem,
    out_send,
    out_recv,
    pass_buf,
    pass_sem,
):
    section = lax.axis_index("section")
    me = lax.axis_index("ctx")
    p = lax.rem(me, 2)
    chip = me // 2
    chips = n // 2
    heads, hd = held.shape[0], held.shape[4]
    rows = held.shape[3]
    slots = held.shape[2]
    back = (slots - 2) // 2
    width = out_buf.shape[3]
    groups = width // hd
    all_heads = 2 * heads
    kv_width = all_heads * hd
    detour = chips == 4
    sibling = me + 1 - 2 * p
    following = lax.rem(section + 1, sections)
    previous = lax.rem(section + sections - 1, sections)

    def cols(start, size):
        return pl.ds(pl.multiple_of(start, hd), size)

    barrier = pltpu.get_barrier_semaphore()

    def greet(sec, ctx):
        pl.semaphore_signal(barrier, inc=1, device_id=(sec, ctx), device_id_type=MESH)

    own_copies = (
        pltpu.make_async_copy(k_hbm, own.at[0], own_sem),
        pltpu.make_async_copy(v_hbm, own.at[1], own_sem),
    )

    def mine_copies(i):
        at = cols((p * heads + i) * hd, hd)
        slot = slots - 2 + p
        return (
            pltpu.make_async_copy(k_hbm.at[:, at], held.at[i, 0, slot], mine_sem),
            pltpu.make_async_copy(v_hbm.at[:, at], held.at[i, 1, slot], mine_sem),
        )

    span = heads * width
    q_copies = (
        pltpu.make_async_copy(q_hbm.at[:, cols(p * span, span)], q_buf.at[p], q_sem.at[0]),
        pltpu.make_async_copy(q_hbm.at[:, cols((1 - p) * span, span)], q_send, q_sem.at[1]),
    )
    reach = heads * hd
    cache_copies = (
        pltpu.make_async_copy(
            cache_hbm.at[:, cols(p * reach, reach)], cache_buf.at[0], cache_sem
        ),
        pltpu.make_async_copy(
            cache_hbm.at[:, cols(kv_width + p * reach, reach)], cache_buf.at[1], cache_sem
        ),
    )
    small = (
        pltpu.make_async_copy(docs_hbm, docs_ref, small_sem.at[0]),
        pltpu.make_async_copy(signs_hbm, signs_ref, small_sem.at[1]),
    )
    def all_of(ref, sem):
        return pltpu.make_async_remote_copy(
            src_ref=ref,
            dst_ref=ref,
            send_sem=sem,
            recv_sem=sem,
            device_id=(section, sibling),
            device_id_type=MESH,
        )

    for copy in own_copies:
        copy.start()

    for d in range(back, 0, -1):
        come = chip >= d
        if detour and d == 1:
            come = come & ((chip != 2) | (p == 0))

        @pl.when(come)
        def _(d=d):
            greet(section, 2 * (chip - d))
            greet(section, 2 * (chip - d) + 1)
    if detour:
        @pl.when(chip == 2)
        def _():
            greet(section, me + 2)

        @pl.when(chip == 0)
        def _():
            greet(section, me + 4)
    greet(section, sibling)
    greet(previous, 2 * chip)
    greet(previous, 2 * chip + 1)

    for copy in small + mine_copies(0) + cache_copies + q_copies:
        copy.start()
    for i in range(1, heads):
        for copy in mine_copies(i):
            copy.start()

    for d in range(1, back + 1):
        @pl.when(chip < d)
        def _(d=d):
            for i in range(heads):
                at = slots - 2 - 2 * d
                held[i, :, at : at + 2] = jnp.zeros((2, 2, rows, hd), held.dtype)

    low = lax.broadcasted_iota(jnp.int32, (hd, hd), 0) & lax.broadcasted_iota(
        jnp.int32, (hd, hd), 1
    )
    shift = 1
    while 2 * shift < hd:
        shift *= 2
    while shift:
        low = low ^ (low >> shift)
        shift //= 2
    hada = (1 - 2 * (low & 1)).astype(jnp.float32).astype(jnp.bfloat16)

    count = jnp.int32(3)
    for d in range(1, back + 1):
        count = count + jnp.where(chip + d < chips, 2, 0)
    if detour:
        count = count + jnp.where(chip >= 2, 1, 0) - jnp.where(chip == 1, 1, 0)
    pl.semaphore_wait(barrier, count)

    def remote(src, dst, index, i, pair, target):
        return pltpu.make_async_remote_copy(
            src_ref=src,
            dst_ref=dst,
            send_sem=send_sem.at[index],
            recv_sem=recv_sem.at[i, pair],
            device_id=(section, target),
            device_id_type=MESH,
        )

    swap_q = pltpu.make_async_remote_copy(
        src_ref=q_send,
        dst_ref=q_buf.at[p],
        send_sem=swap_send,
        recv_sem=swap_recv,
        device_id=(section, sibling),
        device_id_type=MESH,
    )

    def piece(h):
        return own.at[:, :, cols(h * hd, hd)]

    def swap_kv(i):
        block = piece((1 - p) * heads + i)
        return remote(block, held.at[i, :, slots - 2 + p], 0, i, back, sibling)

    def ahead(i):
        for core in range(2):
            for d in range(1, back + 1):
                go = chip + d < chips
                if detour and d == 1:
                    go = go & ((chip != 1) | (i == 0)) if core == 0 else go & (chip != 1)

                @pl.when(go)
                def _(core=core, d=d):
                    slot = slots - 2 - 2 * d + p
                    block = piece(core * heads + i)
                    target = 2 * (chip + d) + core
                    remote(
                        block, held.at[i, :, slot], 2 * d - 1 + core, i, back - d, target
                    ).start()

    def relay_copy(i):
        return remote(held.at[i, :, 0:2], held.at[i, :, 2:4], 1, i, 1, me - 2)

    def arrived(i, pair):
        block = held.at[i, :, 2 * pair : 2 * pair + 2]
        remote(block, block, 0, i, pair, sibling).wait_recv()

    relays = (chip == chips - 1) if detour else False

    def relay(i):
        if detour:
            @pl.when(relays)
            def _():
                arrived(i, 0)

                @pl.when((i > 0) | (p == 1))
                def _():
                    relay_copy(i).start()

    def send(i, carry):
        swap_kv(i).start()
        ahead(i)
        return carry

    all_of(own, own_sem).wait_recv()
    lax.fori_loop(0, heads, send, 0)
    q_copies[1].wait()
    swap_q.start()

    for copy in small:
        copy.wait()
    root = hd ** -0.5
    sign_k = signs_ref[0:1, :].astype(jnp.float32) * root
    sign_v = signs_ref[1:2, :].astype(jnp.float32) * root
    factor = root * float(np.log2(np.e))
    causal = lax.broadcasted_iota(jnp.int32, (rows, rows), 1) <= lax.broadcasted_iota(
        jnp.int32, (rows, rows), 0
    )

    def out_copy(i, e):
        return pltpu.make_async_remote_copy(
            src_ref=out_buf.at[i, e],
            dst_ref=out_ref.at[:, cols((p * heads + i) * width, width)],
            send_sem=out_send,
            recv_sem=out_recv,
            device_id=(following, 2 * chip + e),
            device_id_type=MESH,
        )

    def first_copy(g):
        return pltpu.make_async_remote_copy(
            src_ref=out_buf.at[0, p, :, g * hd : (g + 1) * hd],
            dst_ref=out_ref.at[:, cols(p * heads * width + g * hd, hd)],
            send_sem=out_send,
            recv_sem=out_recv,
            device_id=(following, me),
            device_id_type=MESH,
        )

    def hop(src, dst, sem, recv, target):
        return pltpu.make_async_remote_copy(
            src_ref=src,
            dst_ref=dst,
            send_sem=sem,
            recv_sem=recv,
            device_id=target,
            device_id_type=MESH,
        )

    lent, held_back = LENT
    lender = (chip == 2) if detour else False
    lent_half = lent % 2
    lent_e = (p + lent_half) - 2 * p * lent_half
    lent_out = out_ref.at[:, cols((p * heads + lent // 2) * width, width)]

    def lend():
        return hop(
            out_buf.at[lent // 2, lent_e], pass_buf.at[0], out_send, pass_sem.at[0], (section, p)
        )

    def carry_on():
        return hop(
            pass_buf.at[0], pass_buf.at[1], pass_sem.at[1], pass_sem.at[2], (following, me)
        )

    def hand_over():
        return hop(pass_buf.at[1], lent_out, pass_sem.at[3], out_recv, (section, 4 + lent_e))

    def step(t, carry):
        i = t // 2
        half = lax.rem(t, 2)
        e = (p + half) - 2 * p * half

        @pl.when(t == 0)
        def _():
            all_of(cache_buf, cache_sem).wait_recv()
            all_of(held.at[:, :, slots - 2 + p], mine_sem).wait_recv()
            q_copies[0].wait()

        stretch = 2 * chip + e
        doc = docs_ref[stretch]
        picks = [
            jnp.full((1, hd), jnp.where(doc == k, 1.0, 0.0), jnp.float32).astype(jnp.bfloat16)
            for k in range(cache_buf.shape[1] // CACHE)
        ]

        def cache_block(kind):
            terms = [
                cache_buf[kind, k * CACHE : (k + 1) * CACHE, cols(i * hd, hd)] * pick
                for k, pick in enumerate(picks)
            ]
            return functools.reduce(jnp.add, terms)

        back_k = jnp.dot(cache_block(0), hada, preferred_element_type=jnp.float32)
        back_v = jnp.dot(cache_block(1), hada, preferred_element_type=jnp.float32)
        back_k = (back_k * sign_k).astype(jnp.bfloat16)
        back_v = (back_v * sign_v).astype(jnp.bfloat16)
        biases = []
        for d in range(slots - 2, 0, -1):
            seen = (stretch >= d) & (docs_ref[jnp.maximum(stretch - d, 0)] == doc)
            biases.append(jnp.where(seen, 0.0, -jnp.inf).astype(jnp.float32))

        @pl.when(half == 0)
        def _():
            for pair in range(back):
                there = chip - back + pair >= 0
                if detour and pair == 0:
                    there = there & (chip != chips - 1)

                @pl.when(there)
                def _(pair=pair):
                    arrived(i, pair)

        @pl.when(half == 1 - p)
        def _():
            block = held.at[i, :, slots - 1 - p]
            remote(block, block, 0, i, back, sibling).wait_recv()

        @pl.when(t == 1)
        def _():
            swap_q.wait_recv()

        span_new = (slots - 1) * rows
        keys = held[i, 0, pl.ds(e, slots - 1)].reshape(span_new, hd)
        values = held[i, 1, pl.ds(e, slots - 1)].reshape(span_new, hd)
        keys = jnp.concatenate([back_k, keys], axis=0)
        values = jnp.concatenate([back_v, values], axis=0)
        for g in range(groups):
            query = q_buf[e, :, cols(i * width + g * hd, hd)]
            scores = lax.dot_general(
                query, keys, (((1,), (1,)), ((), ())), preferred_element_type=jnp.float32
            )
            parts = [scores[:, at : at + rows] for at in range(0, CACHE, rows)]
            for d in range(slots - 2):
                at = CACHE + rows * d
                parts.append(scores[:, at : at + rows] + biases[d])
            parts.append(jnp.where(causal, scores[:, CACHE + span_new - rows :], -jnp.inf))
            top = functools.reduce(jnp.maximum, parts)
            top = jnp.max(top, axis=1, keepdims=True)
            expo = [jnp.exp2((part - top) * factor) for part in parts]
            total = jnp.sum(functools.reduce(jnp.add, expo), axis=1, keepdims=True)
            weights = jnp.concatenate([part.astype(jnp.bfloat16) for part in expo], axis=1)
            summed = jnp.dot(weights, values, preferred_element_type=jnp.float32)
            out_buf[i, e, :, g * hd : (g + 1) * hd] = (summed / total).astype(out_buf.dtype)

            @pl.when(t == 0)
            def _(g=g):
                first_copy(g).start()

        if detour:
            @pl.when((chip == 0) & (t == held_back))
            def _():
                lend().wait_recv()
                carry_on().start()

            @pl.when(lender & (t == lent))
            def _():
                lend().start()

        @pl.when((t > 0) & jnp.logical_not(lender & (t == lent)))
        def _():
            out_copy(i, e).start()

        @pl.when((half == 0) & (i + 1 < heads))
        def _():
            relay(i + 1)

        return carry

    relay(0)
    lax.fori_loop(0, 2 * heads, step, 0)

    if detour:
        @pl.when(chip == 0)
        def _():
            carry_on().wait_recv()
            hand_over().start()

    def leaving(core):
        return own.at[:, :, cols(core * heads * hd, heads * hd)]

    all_of(leaving(1 - p), send_sem.at[0]).wait_send()
    swap_q.wait_send()
    for core in range(2):
        for d in range(1, back + 1):
            go = chip + d < chips
            if detour and d == 1:
                go = go & (chip != 1)

            @pl.when(go)
            def _(core=core, d=d):
                all_of(leaving(core), send_sem.at[2 * d - 1 + core]).wait_send()
    if detour:
        @pl.when(chip == 1)
        def _():
            all_of(piece(0), send_sem.at[1]).wait_send()

        @pl.when(relays & (p == 0))
        def _():
            all_of(held.at[1:, :, 0:2], send_sem.at[1]).wait_send()

        @pl.when(relays & (p == 1))
        def _():
            all_of(held.at[:, :, 0:2], send_sem.at[1]).wait_send()
    if detour:
        @pl.when(chip == 0)
        def _():
            carry_on().wait_send()
            hand_over().wait_send()

    all_of(out_buf, out_send).wait_send()
    all_of(out_ref, out_recv).wait_recv()


def per_device(n, sections, queries, keys_new, values_new, stretch_cache, signs, docs):
    rows, q_width = queries.shape[1:]
    kv_width = keys_new.shape[-1]
    hd = signs.shape[-1]
    all_heads = kv_width // hd
    heads = all_heads // 2
    width = q_width // all_heads
    groups = width // hd
    reach = n // 2
    slots = reach + 2
    cached = stretch_cache.shape[1]
    dtype = queries.dtype
    dma = pltpu.SemaphoreType.DMA
    in_hbm = pl.BlockSpec(memory_space=pltpu.HBM)
    out = pl.pallas_call(
        functools.partial(attention_kernel, n, sections),
        out_shape=pltpu.VMEM((rows, q_width), dtype),
        in_specs=[in_hbm] * 6,
        out_specs=pl.BlockSpec(memory_space=pltpu.VMEM),
        scratch_shapes=[
            pltpu.SMEM(docs.shape, docs.dtype),
            pltpu.VMEM(signs.shape[1:], signs.dtype),
            pltpu.VMEM((2, rows, heads * width), dtype),
            pltpu.VMEM((rows, heads * width), dtype),
            pltpu.VMEM((2, cached, heads * hd), dtype),
            pltpu.VMEM((2, rows, kv_width), dtype),
            pltpu.VMEM((heads, 2, slots, rows, hd), dtype),
            pltpu.VMEM((heads, 2, rows, width), dtype),
            dma((2,)),
            dma,
            dma((2,)),
            dma,
            dma,
            dma,
            dma,
            dma((reach + 1,)),
            dma((heads, reach // 2 + 1)),
            dma,
            dma,
            pltpu.VMEM((2, rows, width), dtype),
            dma((4,)),
        ],
        compiler_params=pltpu.CompilerParams(
            collective_id=0, has_side_effects=True, vmem_limit_bytes=58 * 1024 * 1024
        ),
    )(docs, signs[0], queries[0], keys_new[0], values_new[0], stretch_cache[0])
    return out[None]


def solution(mesh):
    in_specs = (
        P("section", "ctx", None),
        P("section", "ctx", None),
        P("section", "ctx", None),
        P("section", None, None),
        P("section", None, None),
        P(),
    )
    out_specs = P("section", "ctx", None)
    body = functools.partial(per_device, mesh.shape["ctx"], mesh.shape["section"])
    return jax.shard_map(body, mesh=mesh, in_specs=in_specs, out_specs=out_specs, check_vma=False)
```

```python
import functools

import jax
import jax.numpy as jnp
import numpy as np
from jax import lax
from jax.experimental import pallas as pl
from jax.experimental.pallas import tpu as pltpu
from jax.sharding import PartitionSpec as P

CACHE = 256
LENT = (4, 7)
PARTS = 3
MESH = pl.DeviceIdType.MESH


def attention_kernel(
    n,
    sections,
    docs_hbm,
    signs_hbm,
    q_hbm,
    k_hbm,
    v_hbm,
    cache_hbm,
    out_ref,
    docs_ref,
    signs_ref,
    q_buf,
    q_send,
    cache_buf,
    own,
    held,
    out_buf,
    small_sem,
    cache_sem,
    q_sem,
    swap_send,
    swap_recv,
    own_sem,
    mine_sem,
    send_sem,
    recv_sem,
    out_send,
    out_recv,
    pass_buf,
    pass_sem,
):
    section = lax.axis_index("section")
    me = lax.axis_index("ctx")
    p = lax.rem(me, 2)
    chip = me // 2
    chips = n // 2
    heads, hd = held.shape[0], held.shape[4]
    rows = held.shape[3]
    slots = held.shape[2]
    back = (slots - 2) // 2
    width = out_buf.shape[3]
    groups = width // hd
    all_heads = 2 * heads
    kv_width = all_heads * hd
    detour = chips == 4
    sibling = me + 1 - 2 * p
    following = lax.rem(section + 1, sections)
    previous = lax.rem(section + sections - 1, sections)

    def cols(start, size):
        return pl.ds(pl.multiple_of(start, hd), size)

    barrier = pltpu.get_barrier_semaphore()

    def greet(sec, ctx):
        pl.semaphore_signal(barrier, inc=1, device_id=(sec, ctx), device_id_type=MESH)

    own_copies = (
        pltpu.make_async_copy(k_hbm, own.at[0], own_sem),
        pltpu.make_async_copy(v_hbm, own.at[1], own_sem),
    )

    def mine_copies(i):
        at = cols((p * heads + i) * hd, hd)
        slot = slots - 2 + p
        return (
            pltpu.make_async_copy(k_hbm.at[:, at], held.at[i, 0, slot], mine_sem),
            pltpu.make_async_copy(v_hbm.at[:, at], held.at[i, 1, slot], mine_sem),
        )

    span = heads * width
    q_copies = (
        pltpu.make_async_copy(q_hbm.at[:, cols(p * span, span)], q_buf.at[p], q_sem.at[0]),
        pltpu.make_async_copy(q_hbm.at[:, cols((1 - p) * span, span)], q_send, q_sem.at[1]),
    )
    reach = heads * hd
    cache_copies = (
        pltpu.make_async_copy(
            cache_hbm.at[:, cols(p * reach, reach)], cache_buf.at[0], cache_sem
        ),
        pltpu.make_async_copy(
            cache_hbm.at[:, cols(kv_width + p * reach, reach)], cache_buf.at[1], cache_sem
        ),
    )
    small = (
        pltpu.make_async_copy(docs_hbm, docs_ref, small_sem.at[0]),
        pltpu.make_async_copy(signs_hbm, signs_ref, small_sem.at[1]),
    )
    def all_of(ref, sem):
        return pltpu.make_async_remote_copy(
            src_ref=ref,
            dst_ref=ref,
            send_sem=sem,
            recv_sem=sem,
            device_id=(section, sibling),
            device_id_type=MESH,
        )

    for copy in own_copies:
        copy.start()

    for d in range(back, 0, -1):
        come = chip >= d
        @pl.when(come)
        def _(d=d):
            greet(section, 2 * (chip - d))
            greet(section, 2 * (chip - d) + 1)
    if detour:
        @pl.when(chip == 2)
        def _():
            greet(section, me + 2)

        @pl.when(chip == 0)
        def _():
            greet(section, me + 4)
    greet(section, sibling)
    greet(previous, 2 * chip)
    greet(previous, 2 * chip + 1)

    for copy in small + mine_copies(0) + cache_copies + q_copies:
        copy.start()
    for i in range(1, heads):
        for copy in mine_copies(i):
            copy.start()

    for d in range(1, back + 1):
        @pl.when(chip < d)
        def _(d=d):
            for i in range(heads):
                at = slots - 2 - 2 * d
                held[i, :, at : at + 2] = jnp.zeros((2, 2, rows, hd), held.dtype)

    low = lax.broadcasted_iota(jnp.int32, (hd, hd), 0) & lax.broadcasted_iota(
        jnp.int32, (hd, hd), 1
    )
    shift = 1
    while 2 * shift < hd:
        shift *= 2
    while shift:
        low = low ^ (low >> shift)
        shift //= 2
    hada = (1 - 2 * (low & 1)).astype(jnp.float32).astype(jnp.bfloat16)

    count = jnp.int32(3)
    for d in range(1, back + 1):
        count = count + jnp.where(chip + d < chips, 2, 0)
    if detour:
        count = count + jnp.where(chip >= 2, 1, 0)
    pl.semaphore_wait(barrier, count)

    def remote(src, dst, index, i, pair, target):
        return pltpu.make_async_remote_copy(
            src_ref=src,
            dst_ref=dst,
            send_sem=send_sem.at[index],
            recv_sem=recv_sem.at[i, pair],
            device_id=(section, target),
            device_id_type=MESH,
        )

    swap_q = pltpu.make_async_remote_copy(
        src_ref=q_send,
        dst_ref=q_buf.at[p],
        send_sem=swap_send,
        recv_sem=swap_recv,
        device_id=(section, sibling),
        device_id_type=MESH,
    )

    def piece(h):
        return own.at[:, :, cols(h * hd, hd)]

    def swap_kv(i):
        block = piece((1 - p) * heads + i)
        return remote(block, held.at[i, :, slots - 2 + p], 0, i, back, sibling)

    def ahead(i):
        for core in range(2):
            for d in range(1, back + 1):
                go = chip + d < chips
                if detour and d == 1:
                    go = go & ((chip != 1) | (i == 0))

                @pl.when(go)
                def _(core=core, d=d):
                    slot = slots - 2 - 2 * d + p
                    block = piece(core * heads + i)
                    target = 2 * (chip + d) + core
                    remote(
                        block, held.at[i, :, slot], 2 * d - 1 + core, i, back - d, target
                    ).start()

    def relay_copy(i):
        return remote(held.at[i, :, 0:2], held.at[i, :, 2:4], 1, i, 1, me - 2)

    def arrived(i, pair):
        block = held.at[i, :, 2 * pair : 2 * pair + 2]
        remote(block, block, 0, i, pair, sibling).wait_recv()

    relays = (chip == chips - 1) if detour else False

    def relay(i):
        if detour:
            @pl.when(relays)
            def _():
                arrived(i, 0)

                @pl.when(i > 0)
                def _():
                    relay_copy(i).start()

    def send(i, carry):
        swap_kv(i).start()
        ahead(i)
        return carry

    all_of(own, own_sem).wait_recv()
    lax.fori_loop(0, heads, send, 0)
    q_copies[1].wait()
    swap_q.start()

    for copy in small:
        copy.wait()
    root = hd ** -0.5
    sign_k = signs_ref[0:1, :].astype(jnp.float32) * root
    sign_v = signs_ref[1:2, :].astype(jnp.float32) * root
    factor = root * float(np.log2(np.e))
    causal = lax.broadcasted_iota(jnp.int32, (rows, rows), 1) <= lax.broadcasted_iota(
        jnp.int32, (rows, rows), 0
    )

    def out_copy(i, e, start, size):
        return pltpu.make_async_remote_copy(
            src_ref=out_buf.at[i, e, :, start : start + size],
            dst_ref=out_ref.at[:, cols((p * heads + i) * width + start, size)],
            send_sem=out_send,
            recv_sem=out_recv,
            device_id=(following, 2 * chip + e),
            device_id_type=MESH,
        )

    def hop(src, dst, sem, recv, target):
        return pltpu.make_async_remote_copy(
            src_ref=src,
            dst_ref=dst,
            send_sem=sem,
            recv_sem=recv,
            device_id=target,
            device_id_type=MESH,
        )

    lent, held_back = LENT
    lender = (chip == 2) if detour else False
    lent_half = lent % 2
    lent_e = (p + lent_half) - 2 * p * lent_half
    share = pass_buf.shape[2]
    kept = width - share
    lent_out = out_ref.at[:, cols((p * heads + lent // 2) * width + kept, share)]

    def lend():
        return hop(
            out_buf.at[lent // 2, lent_e, :, kept:],
            pass_buf.at[0],
            out_send,
            pass_sem.at[0],
            (section, p),
        )

    def carry_on():
        return hop(
            pass_buf.at[0], pass_buf.at[1], pass_sem.at[1], pass_sem.at[2], (following, me)
        )

    def hand_over():
        return hop(pass_buf.at[1], lent_out, pass_sem.at[3], out_recv, (section, 4 + lent_e))

    def step(t, carry):
        i = t // 2
        half = lax.rem(t, 2)
        e = (p + half) - 2 * p * half
        lends = lender & (t == lent)
        in_parts = (t > 0) & ((t < PARTS) | lends)

        @pl.when(t == 0)
        def _():
            all_of(cache_buf, cache_sem).wait_recv()
            all_of(held.at[:, :, slots - 2 + p], mine_sem).wait_recv()
            q_copies[0].wait()

        stretch = 2 * chip + e
        doc = docs_ref[stretch]
        picks = [
            jnp.full((1, hd), jnp.where(doc == k, 1.0, 0.0), jnp.float32).astype(jnp.bfloat16)
            for k in range(cache_buf.shape[1] // CACHE)
        ]

        def cache_block(kind):
            terms = [
                cache_buf[kind, k * CACHE : (k + 1) * CACHE, cols(i * hd, hd)] * pick
                for k, pick in enumerate(picks)
            ]
            return functools.reduce(jnp.add, terms)

        back_k = jnp.dot(cache_block(0), hada, preferred_element_type=jnp.float32)
        back_v = jnp.dot(cache_block(1), hada, preferred_element_type=jnp.float32)
        back_k = (back_k * sign_k).astype(jnp.bfloat16)
        back_v = (back_v * sign_v).astype(jnp.bfloat16)
        biases = []
        for d in range(slots - 2, 0, -1):
            seen = (stretch >= d) & (docs_ref[jnp.maximum(stretch - d, 0)] == doc)
            biases.append(jnp.where(seen, 0.0, -jnp.inf).astype(jnp.float32))

        @pl.when(half == 0)
        def _():
            for pair in range(back):
                there = chip - back + pair >= 0
                if detour and pair == 0:
                    there = there & (chip != chips - 1)

                @pl.when(there)
                def _(pair=pair):
                    arrived(i, pair)

        @pl.when(half == 1 - p)
        def _():
            block = held.at[i, :, slots - 1 - p]
            remote(block, block, 0, i, back, sibling).wait_recv()

        @pl.when(t == 1)
        def _():
            swap_q.wait_recv()

        span_new = (slots - 1) * rows
        keys = held[i, 0, pl.ds(e, slots - 1)].reshape(span_new, hd)
        values = held[i, 1, pl.ds(e, slots - 1)].reshape(span_new, hd)
        keys = jnp.concatenate([back_k, keys], axis=0)
        values = jnp.concatenate([back_v, values], axis=0)
        for g in range(groups):
            query = q_buf[e, :, cols(i * width + g * hd, hd)]
            scores = lax.dot_general(
                query, keys, (((1,), (1,)), ((), ())), preferred_element_type=jnp.float32
            )
            parts = [scores[:, at : at + rows] for at in range(0, CACHE, rows)]
            for d in range(slots - 2):
                at = CACHE + rows * d
                parts.append(scores[:, at : at + rows] + biases[d])
            parts.append(jnp.where(causal, scores[:, CACHE + span_new - rows :], -jnp.inf))
            top = functools.reduce(jnp.maximum, parts)
            top = jnp.max(top, axis=1, keepdims=True)
            expo = [jnp.exp2((part - top) * factor) for part in parts]
            total = jnp.sum(functools.reduce(jnp.add, expo), axis=1, keepdims=True)
            weights = jnp.concatenate([part.astype(jnp.bfloat16) for part in expo], axis=1)
            summed = jnp.dot(weights, values, preferred_element_type=jnp.float32)
            out_buf[i, e, :, g * hd : (g + 1) * hd] = (summed / total).astype(out_buf.dtype)

            @pl.when(t == 0)
            def _(g=g):
                out_copy(i, e, g * hd, hd).start()

            if g == groups // 2 - 1:
                @pl.when(in_parts)
                def _():
                    out_copy(i, e, 0, width // 2).start()

        if detour:
            @pl.when((chip == 0) & (t == held_back))
            def _():
                lend().wait_recv()
                carry_on().start()

            @pl.when(lends)
            def _():
                lend().start()

        @pl.when(in_parts & jnp.logical_not(lends))
        def _():
            out_copy(i, e, width // 2, width // 2).start()

        @pl.when((t >= PARTS) & jnp.logical_not(lends))
        def _():
            out_copy(i, e, 0, width).start()

        @pl.when((half == 0) & (i + 1 < heads))
        def _():
            relay(i + 1)

        return carry

    relay(0)
    lax.fori_loop(0, 2 * heads, step, 0)

    if detour:
        @pl.when(chip == 0)
        def _():
            carry_on().wait_recv()
            hand_over().start()

    def leaving(core):
        return own.at[:, :, cols(core * heads * hd, heads * hd)]

    all_of(leaving(1 - p), send_sem.at[0]).wait_send()
    swap_q.wait_send()
    for core in range(2):
        for d in range(1, back + 1):
            go = chip + d < chips
            if detour and d == 1:
                go = go & (chip != 1)

            @pl.when(go)
            def _(core=core, d=d):
                all_of(leaving(core), send_sem.at[2 * d - 1 + core]).wait_send()
    if detour:
        @pl.when(chip == 1)
        def _():
            for core in range(2):
                all_of(piece(0), send_sem.at[1 + core]).wait_send()

        @pl.when(relays)
        def _():
            all_of(held.at[1:, :, 0:2], send_sem.at[1]).wait_send()
    if detour:
        @pl.when(chip == 0)
        def _():
            carry_on().wait_send()
            hand_over().wait_send()

    all_of(out_buf, out_send).wait_send()
    all_of(out_ref, out_recv).wait_recv()


def per_device(n, sections, queries, keys_new, values_new, stretch_cache, signs, docs):
    rows, q_width = queries.shape[1:]
    kv_width = keys_new.shape[-1]
    hd = signs.shape[-1]
    all_heads = kv_width // hd
    heads = all_heads // 2
    width = q_width // all_heads
    groups = width // hd
    reach = n // 2
    slots = reach + 2
    cached = stretch_cache.shape[1]
    dtype = queries.dtype
    dma = pltpu.SemaphoreType.DMA
    in_hbm = pl.BlockSpec(memory_space=pltpu.HBM)
    out = pl.pallas_call(
        functools.partial(attention_kernel, n, sections),
        out_shape=pltpu.VMEM((rows, q_width), dtype),
        in_specs=[in_hbm] * 6,
        out_specs=pl.BlockSpec(memory_space=pltpu.VMEM),
        scratch_shapes=[
            pltpu.SMEM(docs.shape, docs.dtype),
            pltpu.VMEM(signs.shape[1:], signs.dtype),
            pltpu.VMEM((2, rows, heads * width), dtype),
            pltpu.VMEM((rows, heads * width), dtype),
            pltpu.VMEM((2, cached, heads * hd), dtype),
            pltpu.VMEM((2, rows, kv_width), dtype),
            pltpu.VMEM((heads, 2, slots, rows, hd), dtype),
            pltpu.VMEM((heads, 2, rows, width), dtype),
            dma((2,)),
            dma,
            dma((2,)),
            dma,
            dma,
            dma,
            dma,
            dma((reach + 1,)),
            dma((heads, reach // 2 + 1)),
            dma,
            dma,
            pltpu.VMEM((2, rows, width // 2), dtype),
            dma((4,)),
        ],
        compiler_params=pltpu.CompilerParams(
            collective_id=0, has_side_effects=True, vmem_limit_bytes=58 * 1024 * 1024
        ),
    )(docs, signs[0], queries[0], keys_new[0], values_new[0], stretch_cache[0])
    return out[None]


def solution(mesh):
    in_specs = (
        P("section", "ctx", None),
        P("section", "ctx", None),
        P("section", "ctx", None),
        P("section", None, None),
        P("section", None, None),
        P(),
    )
    out_specs = P("section", "ctx", None)
    body = functools.partial(per_device, mesh.shape["ctx"], mesh.shape["section"])
    return jax.shard_map(body, mesh=mesh, in_specs=in_specs, out_specs=out_specs, check_vma=False)
```

```python
import functools

import jax
import jax.numpy as jnp
import numpy as np
from jax import lax
from jax.experimental import pallas as pl
from jax.experimental.pallas import tpu as pltpu
from jax.sharding import PartitionSpec as P

CACHE = 256
LENT = (4, 7)
PARTS = 3
MESH = pl.DeviceIdType.MESH


def attention_kernel(
    n,
    sections,
    docs_hbm,
    signs_hbm,
    q_hbm,
    k_hbm,
    v_hbm,
    cache_hbm,
    out_ref,
    docs_ref,
    signs_ref,
    q_buf,
    q_send,
    cache_buf,
    own,
    held,
    out_buf,
    small_sem,
    cache_sem,
    q_sem,
    swap_send,
    swap_recv,
    own_sem,
    mine_sem,
    send_sem,
    recv_sem,
    out_send,
    out_recv,
    pass_buf,
    pass_sem,
):
    section = lax.axis_index("section")
    me = lax.axis_index("ctx")
    p = lax.rem(me, 2)
    chip = me // 2
    chips = n // 2
    heads, hd = held.shape[0], held.shape[4]
    rows = held.shape[3]
    slots = held.shape[2]
    back = (slots - 2) // 2
    width = out_buf.shape[3]
    groups = width // hd
    all_heads = 2 * heads
    kv_width = all_heads * hd
    detour = chips == 4
    sibling = me + 1 - 2 * p
    following = lax.rem(section + 1, sections)
    previous = lax.rem(section + sections - 1, sections)

    def cols(start, size):
        return pl.ds(pl.multiple_of(start, hd), size)

    barrier = pltpu.get_barrier_semaphore()

    def greet(sec, ctx):
        pl.semaphore_signal(barrier, inc=1, device_id=(sec, ctx), device_id_type=MESH)

    own_copies = (
        pltpu.make_async_copy(k_hbm, own.at[0], own_sem),
        pltpu.make_async_copy(v_hbm, own.at[1], own_sem),
    )

    def mine_copies(i):
        at = cols((p * heads + i) * hd, hd)
        slot = slots - 2 + p
        return (
            pltpu.make_async_copy(k_hbm.at[:, at], held.at[i, 0, slot], mine_sem),
            pltpu.make_async_copy(v_hbm.at[:, at], held.at[i, 1, slot], mine_sem),
        )

    span = heads * width
    q_copies = (
        pltpu.make_async_copy(q_hbm.at[:, cols(p * span, span)], q_buf.at[p], q_sem.at[0]),
        pltpu.make_async_copy(q_hbm.at[:, cols((1 - p) * span, span)], q_send, q_sem.at[1]),
    )
    reach = heads * hd
    cache_copies = (
        pltpu.make_async_copy(
            cache_hbm.at[:, cols(p * reach, reach)], cache_buf.at[0], cache_sem
        ),
        pltpu.make_async_copy(
            cache_hbm.at[:, cols(kv_width + p * reach, reach)], cache_buf.at[1], cache_sem
        ),
    )
    small = (
        pltpu.make_async_copy(docs_hbm, docs_ref, small_sem.at[0]),
        pltpu.make_async_copy(signs_hbm, signs_ref, small_sem.at[1]),
    )
    def all_of(ref, sem):
        return pltpu.make_async_remote_copy(
            src_ref=ref,
            dst_ref=ref,
            send_sem=sem,
            recv_sem=sem,
            device_id=(section, sibling),
            device_id_type=MESH,
        )

    for copy in own_copies:
        copy.start()

    for d in range(back, 0, -1):
        come = chip >= d
        @pl.when(come)
        def _(d=d):
            greet(section, 2 * (chip - d))
            greet(section, 2 * (chip - d) + 1)
    if detour:
        @pl.when(chip == 2)
        def _():
            greet(section, me + 2)

        @pl.when(chip == 0)
        def _():
            greet(section, me + 4)
    greet(section, sibling)
    greet(previous, 2 * chip)
    greet(previous, 2 * chip + 1)

    for copy in small + mine_copies(0) + cache_copies + q_copies:
        copy.start()
    for i in range(1, heads):
        for copy in mine_copies(i):
            copy.start()

    for d in range(1, back + 1):
        @pl.when(chip < d)
        def _(d=d):
            for i in range(heads):
                at = slots - 2 - 2 * d
                held[i, :, at : at + 2] = jnp.zeros((2, 2, rows, hd), held.dtype)

    low = lax.broadcasted_iota(jnp.int32, (hd, hd), 0) & lax.broadcasted_iota(
        jnp.int32, (hd, hd), 1
    )
    shift = 1
    while 2 * shift < hd:
        shift *= 2
    while shift:
        low = low ^ (low >> shift)
        shift //= 2
    hada = (1 - 2 * (low & 1)).astype(jnp.float32).astype(jnp.bfloat16)

    count = jnp.int32(3)
    for d in range(1, back + 1):
        count = count + jnp.where(chip + d < chips, 2, 0)
    if detour:
        count = count + jnp.where(chip >= 2, 1, 0)
    pl.semaphore_wait(barrier, count)

    def remote(src, dst, index, i, pair, target):
        return pltpu.make_async_remote_copy(
            src_ref=src,
            dst_ref=dst,
            send_sem=send_sem.at[index],
            recv_sem=recv_sem.at[i, pair],
            device_id=(section, target),
            device_id_type=MESH,
        )

    swap_q = pltpu.make_async_remote_copy(
        src_ref=q_send,
        dst_ref=q_buf.at[p],
        send_sem=swap_send,
        recv_sem=swap_recv,
        device_id=(section, sibling),
        device_id_type=MESH,
    )

    def piece(h):
        return own.at[:, :, cols(h * hd, hd)]

    def swap_kv(i):
        block = piece((1 - p) * heads + i)
        return remote(block, held.at[i, :, slots - 2 + p], 0, i, back, sibling)

    def ahead(i, core):
        for d in range(1, back + 1):
            go = chip + d < chips
            if detour and d == 1:
                go = go & ((chip != 1) | (i == 0))

            @pl.when(go)
            def _(d=d):
                slot = slots - 2 - 2 * d + p
                block = piece(core * heads + i)
                target = 2 * (chip + d) + core
                remote(
                    block, held.at[i, :, slot], 2 * d - 1 + core, i, back - d, target
                ).start()

    def relay_copy(i):
        return remote(held.at[i, :, 0:2], held.at[i, :, 2:4], 1, i, 1, me - 2)

    def arrived(i, pair):
        block = held.at[i, :, 2 * pair : 2 * pair + 2]
        remote(block, block, 0, i, pair, sibling).wait_recv()

    relays = (chip == chips - 1) if detour else False

    def relay(i):
        if detour:
            @pl.when(relays)
            def _():
                arrived(i, 0)

                @pl.when(i > 0)
                def _():
                    relay_copy(i).start()

    def send(k, carry):
        i, core = k // 2, lax.rem(k, 2)
        if detour and heads % 2 == 0:
            pairs = chip == 1
            i = jnp.where(pairs, 2 * (k // 4) + lax.rem(k, 2), i)
            core = jnp.where(pairs, lax.rem(k // 2, 2), core)

        @pl.when(core == 0)
        def _():
            swap_kv(i).start()

        ahead(i, core)
        return carry

    all_of(own, own_sem).wait_recv()
    lax.fori_loop(0, 2 * heads, send, 0)
    q_copies[1].wait()
    swap_q.start()

    for copy in small:
        copy.wait()
    root = hd ** -0.5
    sign_k = signs_ref[0:1, :].astype(jnp.float32) * root
    sign_v = signs_ref[1:2, :].astype(jnp.float32) * root
    factor = root * float(np.log2(np.e))
    causal = lax.broadcasted_iota(jnp.int32, (rows, rows), 1) <= lax.broadcasted_iota(
        jnp.int32, (rows, rows), 0
    )

    def out_copy(i, e, start, size):
        return pltpu.make_async_remote_copy(
            src_ref=out_buf.at[i, e, :, start : start + size],
            dst_ref=out_ref.at[:, cols((p * heads + i) * width + start, size)],
            send_sem=out_send,
            recv_sem=out_recv,
            device_id=(following, 2 * chip + e),
            device_id_type=MESH,
        )

    def hop(src, dst, sem, recv, target):
        return pltpu.make_async_remote_copy(
            src_ref=src,
            dst_ref=dst,
            send_sem=sem,
            recv_sem=recv,
            device_id=target,
            device_id_type=MESH,
        )

    lent, held_back = LENT
    lender = (chip == 2) if detour else False
    lent_half = lent % 2
    lent_e = (p + lent_half) - 2 * p * lent_half
    share = pass_buf.shape[2]
    kept = width - share
    lent_out = out_ref.at[:, cols((p * heads + lent // 2) * width + kept, share)]

    def lend():
        return hop(
            out_buf.at[lent // 2, lent_e, :, kept:],
            pass_buf.at[0],
            out_send,
            pass_sem.at[0],
            (section, p),
        )

    def carry_on():
        return hop(
            pass_buf.at[0], pass_buf.at[1], pass_sem.at[1], pass_sem.at[2], (following, me)
        )

    def hand_over():
        return hop(pass_buf.at[1], lent_out, pass_sem.at[3], out_recv, (section, 4 + lent_e))

    def step(t, carry):
        i = t // 2
        half = lax.rem(t, 2)
        e = (p + half) - 2 * p * half
        lends = lender & (t == lent)
        in_parts = (t > 0) & ((t < PARTS) | lends)

        @pl.when(t == 0)
        def _():
            all_of(cache_buf, cache_sem).wait_recv()
            all_of(held.at[:, :, slots - 2 + p], mine_sem).wait_recv()
            q_copies[0].wait()

        stretch = 2 * chip + e
        doc = docs_ref[stretch]
        picks = [
            jnp.full((1, hd), jnp.where(doc == k, 1.0, 0.0), jnp.float32).astype(jnp.bfloat16)
            for k in range(cache_buf.shape[1] // CACHE)
        ]

        def cache_block(kind):
            terms = [
                cache_buf[kind, k * CACHE : (k + 1) * CACHE, cols(i * hd, hd)] * pick
                for k, pick in enumerate(picks)
            ]
            return functools.reduce(jnp.add, terms)

        back_k = jnp.dot(cache_block(0), hada, preferred_element_type=jnp.float32)
        back_v = jnp.dot(cache_block(1), hada, preferred_element_type=jnp.float32)
        back_k = (back_k * sign_k).astype(jnp.bfloat16)
        back_v = (back_v * sign_v).astype(jnp.bfloat16)
        biases = []
        for d in range(slots - 2, 0, -1):
            seen = (stretch >= d) & (docs_ref[jnp.maximum(stretch - d, 0)] == doc)
            biases.append(jnp.where(seen, 0.0, -jnp.inf).astype(jnp.float32))

        @pl.when(half == 0)
        def _():
            for pair in range(back):
                there = chip - back + pair >= 0
                if detour and pair == 0:
                    there = there & (chip != chips - 1)

                @pl.when(there)
                def _(pair=pair):
                    arrived(i, pair)

        @pl.when(half == 1 - p)
        def _():
            block = held.at[i, :, slots - 1 - p]
            remote(block, block, 0, i, back, sibling).wait_recv()

        @pl.when(t == 1)
        def _():
            swap_q.wait_recv()

        span_new = (slots - 1) * rows
        keys = held[i, 0, pl.ds(e, slots - 1)].reshape(span_new, hd)
        values = held[i, 1, pl.ds(e, slots - 1)].reshape(span_new, hd)
        keys = jnp.concatenate([back_k, keys], axis=0)
        values = jnp.concatenate([back_v, values], axis=0)
        for g in range(groups):
            query = q_buf[e, :, cols(i * width + g * hd, hd)]
            scores = lax.dot_general(
                query, keys, (((1,), (1,)), ((), ())), preferred_element_type=jnp.float32
            )
            parts = [scores[:, at : at + rows] for at in range(0, CACHE, rows)]
            for d in range(slots - 2):
                at = CACHE + rows * d
                parts.append(scores[:, at : at + rows] + biases[d])
            parts.append(jnp.where(causal, scores[:, CACHE + span_new - rows :], -jnp.inf))
            top = functools.reduce(jnp.maximum, parts)
            top = jnp.max(top, axis=1, keepdims=True)
            expo = [jnp.exp2((part - top) * factor) for part in parts]
            total = jnp.sum(functools.reduce(jnp.add, expo), axis=1, keepdims=True)
            weights = jnp.concatenate([part.astype(jnp.bfloat16) for part in expo], axis=1)
            summed = jnp.dot(weights, values, preferred_element_type=jnp.float32)
            out_buf[i, e, :, g * hd : (g + 1) * hd] = (summed / total).astype(out_buf.dtype)

            @pl.when(t == 0)
            def _(g=g):
                out_copy(i, e, g * hd, hd).start()

            if g == groups // 2 - 1:
                @pl.when(in_parts)
                def _():
                    out_copy(i, e, 0, width // 2).start()

        if detour:
            @pl.when((chip == 0) & (t == held_back))
            def _():
                lend().wait_recv()
                carry_on().start()

            @pl.when(lends)
            def _():
                lend().start()

        @pl.when(in_parts & jnp.logical_not(lends))
        def _():
            out_copy(i, e, width // 2, width // 2).start()

        @pl.when((t >= PARTS) & jnp.logical_not(lends))
        def _():
            out_copy(i, e, 0, width).start()

        @pl.when((half == 0) & (i + 1 < heads))
        def _():
            relay(i + 1)

        return carry

    relay(0)
    lax.fori_loop(0, 2 * heads, step, 0)

    if detour:
        @pl.when(chip == 0)
        def _():
            carry_on().wait_recv()
            hand_over().start()

    def leaving(core):
        return own.at[:, :, cols(core * heads * hd, heads * hd)]

    all_of(leaving(1 - p), send_sem.at[0]).wait_send()
    swap_q.wait_send()
    for core in range(2):
        for d in range(1, back + 1):
            go = chip + d < chips
            if detour and d == 1:
                go = go & (chip != 1)

            @pl.when(go)
            def _(core=core, d=d):
                all_of(leaving(core), send_sem.at[2 * d - 1 + core]).wait_send()
    if detour:
        @pl.when(chip == 1)
        def _():
            for core in range(2):
                all_of(piece(0), send_sem.at[1 + core]).wait_send()

        @pl.when(relays)
        def _():
            all_of(held.at[1:, :, 0:2], send_sem.at[1]).wait_send()
    if detour:
        @pl.when(chip == 0)
        def _():
            carry_on().wait_send()
            hand_over().wait_send()

    all_of(out_buf, out_send).wait_send()
    all_of(out_ref, out_recv).wait_recv()


def per_device(n, sections, queries, keys_new, values_new, stretch_cache, signs, docs):
    rows, q_width = queries.shape[1:]
    kv_width = keys_new.shape[-1]
    hd = signs.shape[-1]
    all_heads = kv_width // hd
    heads = all_heads // 2
    width = q_width // all_heads
    groups = width // hd
    reach = n // 2
    slots = reach + 2
    cached = stretch_cache.shape[1]
    dtype = queries.dtype
    dma = pltpu.SemaphoreType.DMA
    in_hbm = pl.BlockSpec(memory_space=pltpu.HBM)
    out = pl.pallas_call(
        functools.partial(attention_kernel, n, sections),
        out_shape=pltpu.VMEM((rows, q_width), dtype),
        in_specs=[in_hbm] * 6,
        out_specs=pl.BlockSpec(memory_space=pltpu.VMEM),
        scratch_shapes=[
            pltpu.SMEM(docs.shape, docs.dtype),
            pltpu.VMEM(signs.shape[1:], signs.dtype),
            pltpu.VMEM((2, rows, heads * width), dtype),
            pltpu.VMEM((rows, heads * width), dtype),
            pltpu.VMEM((2, cached, heads * hd), dtype),
            pltpu.VMEM((2, rows, kv_width), dtype),
            pltpu.VMEM((heads, 2, slots, rows, hd), dtype),
            pltpu.VMEM((heads, 2, rows, width), dtype),
            dma((2,)),
            dma,
            dma((2,)),
            dma,
            dma,
            dma,
            dma,
            dma((reach + 1,)),
            dma((heads, reach // 2 + 1)),
            dma,
            dma,
            pltpu.VMEM((2, rows, width // 2), dtype),
            dma((4,)),
        ],
        compiler_params=pltpu.CompilerParams(
            collective_id=0, has_side_effects=True, vmem_limit_bytes=58 * 1024 * 1024
        ),
    )(docs, signs[0], queries[0], keys_new[0], values_new[0], stretch_cache[0])
    return out[None]


def solution(mesh):
    in_specs = (
        P("section", "ctx", None),
        P("section", "ctx", None),
        P("section", "ctx", None),
        P("section", None, None),
        P("section", None, None),
        P(),
    )
    out_specs = P("section", "ctx", None)
    body = functools.partial(per_device, mesh.shape["ctx"], mesh.shape["section"])
    return jax.shard_map(body, mesh=mesh, in_specs=in_specs, out_specs=out_specs, check_vma=False)
```

```python
import functools

import jax
import jax.numpy as jnp
import numpy as np
from jax import lax
from jax.experimental import pallas as pl
from jax.experimental.pallas import tpu as pltpu
from jax.sharding import PartitionSpec as P

CACHE = 256
LENT = (4, 7)
PARTS = 3
MESH = pl.DeviceIdType.MESH


def attention_kernel(
    n,
    sections,
    docs_hbm,
    signs_hbm,
    q_hbm,
    k_hbm,
    v_hbm,
    cache_hbm,
    out_ref,
    docs_ref,
    signs_ref,
    q_buf,
    q_send,
    cache_buf,
    own,
    held,
    out_buf,
    small_sem,
    cache_sem,
    q_sem,
    swap_send,
    swap_recv,
    own_sem,
    mine_sem,
    send_sem,
    recv_sem,
    out_send,
    out_recv,
    pass_buf,
    pass_sem,
):
    section = lax.axis_index("section")
    me = lax.axis_index("ctx")
    p = lax.rem(me, 2)
    chip = me // 2
    chips = n // 2
    heads, hd = held.shape[0], held.shape[4]
    rows = held.shape[3]
    slots = held.shape[2]
    back = (slots - 2) // 2
    width = out_buf.shape[3]
    groups = width // hd
    all_heads = 2 * heads
    kv_width = all_heads * hd
    detour = chips == 4
    sibling = me + 1 - 2 * p
    following = lax.rem(section + 1, sections)
    previous = lax.rem(section + sections - 1, sections)

    def cols(start, size):
        return pl.ds(pl.multiple_of(start, hd), size)

    barrier = pltpu.get_barrier_semaphore()

    def greet(sec, ctx):
        pl.semaphore_signal(barrier, inc=1, device_id=(sec, ctx), device_id_type=MESH)

    own_copies = (
        pltpu.make_async_copy(k_hbm, own.at[0], own_sem),
        pltpu.make_async_copy(v_hbm, own.at[1], own_sem),
    )

    def mine_copies(i):
        at = cols((p * heads + i) * hd, hd)
        slot = slots - 2 + p
        return (
            pltpu.make_async_copy(k_hbm.at[:, at], held.at[i, 0, slot], mine_sem),
            pltpu.make_async_copy(v_hbm.at[:, at], held.at[i, 1, slot], mine_sem),
        )

    span = heads * width
    q_copies = (
        pltpu.make_async_copy(q_hbm.at[:, cols(p * span, span)], q_buf.at[p], q_sem.at[0]),
        pltpu.make_async_copy(q_hbm.at[:, cols((1 - p) * span, span)], q_send, q_sem.at[1]),
    )
    reach = heads * hd
    cache_copies = (
        pltpu.make_async_copy(
            cache_hbm.at[:, cols(p * reach, reach)], cache_buf.at[0], cache_sem
        ),
        pltpu.make_async_copy(
            cache_hbm.at[:, cols(kv_width + p * reach, reach)], cache_buf.at[1], cache_sem
        ),
    )
    small = (
        pltpu.make_async_copy(docs_hbm, docs_ref, small_sem.at[0]),
        pltpu.make_async_copy(signs_hbm, signs_ref, small_sem.at[1]),
    )
    def all_of(ref, sem):
        return pltpu.make_async_remote_copy(
            src_ref=ref,
            dst_ref=ref,
            send_sem=sem,
            recv_sem=sem,
            device_id=(section, sibling),
            device_id_type=MESH,
        )

    for copy in own_copies:
        copy.start()

    for d in range(back, 0, -1):
        come = chip >= d
        @pl.when(come)
        def _(d=d):
            greet(section, 2 * (chip - d))
            greet(section, 2 * (chip - d) + 1)
    if detour:
        @pl.when(chip == 2)
        def _():
            greet(section, me + 2)

        @pl.when(chip == 0)
        def _():
            greet(section, me + 4)
    greet(section, sibling)
    greet(previous, 2 * chip)
    greet(previous, 2 * chip + 1)

    for copy in small + mine_copies(0) + cache_copies + q_copies:
        copy.start()
    for i in range(1, heads):
        for copy in mine_copies(i):
            copy.start()

    for d in range(1, back + 1):
        @pl.when(chip < d)
        def _(d=d):
            for i in range(heads):
                at = slots - 2 - 2 * d
                held[i, :, at : at + 2] = jnp.zeros((2, 2, rows, hd), held.dtype)

    low = lax.broadcasted_iota(jnp.int32, (hd, hd), 0) & lax.broadcasted_iota(
        jnp.int32, (hd, hd), 1
    )
    shift = 1
    while 2 * shift < hd:
        shift *= 2
    while shift:
        low = low ^ (low >> shift)
        shift //= 2
    hada = (1 - 2 * (low & 1)).astype(jnp.float32).astype(jnp.bfloat16)

    count = jnp.int32(3)
    for d in range(1, back + 1):
        count = count + jnp.where(chip + d < chips, 2, 0)
    if detour:
        count = count + jnp.where(chip >= 2, 1, 0)
    pl.semaphore_wait(barrier, count)

    def remote(src, dst, index, i, pair, target):
        return pltpu.make_async_remote_copy(
            src_ref=src,
            dst_ref=dst,
            send_sem=send_sem.at[index],
            recv_sem=recv_sem.at[i, pair],
            device_id=(section, target),
            device_id_type=MESH,
        )

    swap_q = pltpu.make_async_remote_copy(
        src_ref=q_send,
        dst_ref=q_buf.at[p],
        send_sem=swap_send,
        recv_sem=swap_recv,
        device_id=(section, sibling),
        device_id_type=MESH,
    )

    def piece(h):
        return own.at[:, :, cols(h * hd, hd)]

    def swap_kv(i):
        block = piece((1 - p) * heads + i)
        return remote(block, held.at[i, :, slots - 2 + p], 0, i, back, sibling)

    def ahead(i, core):
        for d in range(1, back + 1):
            go = chip + d < chips
            if detour and d == 1:
                go = go & ((chip != 1) | (i == 0))

            @pl.when(go)
            def _(d=d):
                slot = slots - 2 - 2 * d + p
                block = piece(core * heads + i)
                target = 2 * (chip + d) + core
                remote(
                    block, held.at[i, :, slot], 2 * d - 1 + core, i, back - d, target
                ).start()

    def relay_copy(i):
        return remote(held.at[i, :, 0:2], held.at[i, :, 2:4], 1, i, 1, me - 2)

    def arrived(i, pair):
        block = held.at[i, :, 2 * pair : 2 * pair + 2]
        remote(block, block, 0, i, pair, sibling).wait_recv()

    relays = (chip == chips - 1) if detour else False

    def relay(i):
        if detour:
            @pl.when(relays)
            def _():
                arrived(i, 0)

                @pl.when(i > 0)
                def _():
                    relay_copy(i).start()

    def send(k, carry):
        i, core = k // 2, lax.rem(k, 2)
        if detour and heads % 2 == 0:
            pairs = chip == 1
            i = jnp.where(pairs, 2 * (k // 4) + lax.rem(k, 2), i)
            core = jnp.where(pairs, lax.rem(k // 2, 2), core)

        @pl.when(core == 0)
        def _():
            swap_kv(i).start()

        ahead(i, core)
        return carry

    all_of(own, own_sem).wait_recv()
    lax.fori_loop(0, 2 * heads, send, 0)
    q_copies[1].wait()
    swap_q.start()

    for copy in small:
        copy.wait()
    root = hd ** -0.5
    sign_k = signs_ref[0:1, :].astype(jnp.float32) * root
    sign_v = signs_ref[1:2, :].astype(jnp.float32) * root
    factor = root * float(np.log2(np.e))
    causal = lax.broadcasted_iota(jnp.int32, (rows, rows), 1) <= lax.broadcasted_iota(
        jnp.int32, (rows, rows), 0
    )

    def out_copy(i, e, start, size):
        return pltpu.make_async_remote_copy(
            src_ref=out_buf.at[i, e, :, start : start + size],
            dst_ref=out_ref.at[:, cols((p * heads + i) * width + start, size)],
            send_sem=out_send,
            recv_sem=out_recv,
            device_id=(following, 2 * chip + e),
            device_id_type=MESH,
        )

    def hop(src, dst, sem, recv, target):
        return pltpu.make_async_remote_copy(
            src_ref=src,
            dst_ref=dst,
            send_sem=sem,
            recv_sem=recv,
            device_id=target,
            device_id_type=MESH,
        )

    lent, held_back = LENT
    lender = (chip == 2) if detour else False
    lent_half = lent % 2
    lent_e = (p + lent_half) - 2 * p * lent_half
    share = pass_buf.shape[2]
    kept = width - share
    lent_out = out_ref.at[:, cols((p * heads + lent // 2) * width + kept, share)]

    def lend():
        return hop(
            out_buf.at[lent // 2, lent_e, :, kept:],
            pass_buf.at[0],
            out_send,
            pass_sem.at[0],
            (section, p),
        )

    def carry_on():
        return hop(
            pass_buf.at[0], pass_buf.at[1], pass_sem.at[1], pass_sem.at[2], (following, me)
        )

    def hand_over():
        return hop(pass_buf.at[1], lent_out, pass_sem.at[3], out_recv, (section, 4 + lent_e))

    def step(t, carry):
        i = t // 2
        half = lax.rem(t, 2)
        e = (p + half) - 2 * p * half
        lends = lender & (t == lent)
        in_parts = (t == 1) | lends

        @pl.when(t == 0)
        def _():
            all_of(cache_buf, cache_sem).wait_recv()
            all_of(held.at[:, :, slots - 2 + p], mine_sem).wait_recv()
            q_copies[0].wait()

        stretch = 2 * chip + e
        doc = docs_ref[stretch]
        picks = [
            jnp.full((1, hd), jnp.where(doc == k, 1.0, 0.0), jnp.float32).astype(jnp.bfloat16)
            for k in range(cache_buf.shape[1] // CACHE)
        ]

        def cache_block(kind):
            terms = [
                cache_buf[kind, k * CACHE : (k + 1) * CACHE, cols(i * hd, hd)] * pick
                for k, pick in enumerate(picks)
            ]
            return functools.reduce(jnp.add, terms)

        back_k = jnp.dot(cache_block(0), hada, preferred_element_type=jnp.float32)
        back_v = jnp.dot(cache_block(1), hada, preferred_element_type=jnp.float32)
        back_k = (back_k * sign_k).astype(jnp.bfloat16)
        back_v = (back_v * sign_v).astype(jnp.bfloat16)
        biases = []
        for d in range(slots - 2, 0, -1):
            seen = (stretch >= d) & (docs_ref[jnp.maximum(stretch - d, 0)] == doc)
            biases.append(jnp.where(seen, 0.0, -jnp.inf).astype(jnp.float32))

        @pl.when(half == 0)
        def _():
            for pair in range(back):
                there = chip - back + pair >= 0
                if detour and pair == 0:
                    there = there & (chip != chips - 1)

                @pl.when(there)
                def _(pair=pair):
                    arrived(i, pair)

        @pl.when(half == 1 - p)
        def _():
            block = held.at[i, :, slots - 1 - p]
            remote(block, block, 0, i, back, sibling).wait_recv()

        @pl.when(t == 1)
        def _():
            swap_q.wait_recv()

        span_new = (slots - 1) * rows
        keys = held[i, 0, pl.ds(e, slots - 1)].reshape(span_new, hd)
        values = held[i, 1, pl.ds(e, slots - 1)].reshape(span_new, hd)
        keys = jnp.concatenate([back_k, keys], axis=0)
        values = jnp.concatenate([back_v, values], axis=0)
        for g in range(groups):
            query = q_buf[e, :, cols(i * width + g * hd, hd)]
            scores = lax.dot_general(
                query, keys, (((1,), (1,)), ((), ())), preferred_element_type=jnp.float32
            )
            parts = [scores[:, at : at + rows] for at in range(0, CACHE, rows)]
            for d in range(slots - 2):
                at = CACHE + rows * d
                parts.append(scores[:, at : at + rows] + biases[d])
            parts.append(jnp.where(causal, scores[:, CACHE + span_new - rows :], -jnp.inf))
            top = functools.reduce(jnp.maximum, parts)
            top = jnp.max(top, axis=1, keepdims=True)
            expo = [jnp.exp2((part - top) * factor) for part in parts]
            total = jnp.sum(functools.reduce(jnp.add, expo), axis=1, keepdims=True)
            weights = jnp.concatenate([part.astype(jnp.bfloat16) for part in expo], axis=1)
            summed = jnp.dot(weights, values, preferred_element_type=jnp.float32)
            out_buf[i, e, :, g * hd : (g + 1) * hd] = (summed / total).astype(out_buf.dtype)

            @pl.when((t == 0) | (t == 2))
            def _(g=g):
                out_copy(i, e, g * hd, hd).start()

            if g == groups // 2:
                @pl.when((half == 0) & (i + 1 < heads))
                def _():
                    relay(i + 1)

            if g == groups // 2 - 1:
                @pl.when(in_parts)
                def _():
                    out_copy(i, e, 0, width // 2).start()

        if detour:
            @pl.when((chip == 0) & (t == held_back))
            def _():
                lend().wait_recv()
                carry_on().start()

            @pl.when(lends)
            def _():
                lend().start()

        @pl.when(in_parts & jnp.logical_not(lends))
        def _():
            out_copy(i, e, width // 2, width // 2).start()

        @pl.when((t >= PARTS) & jnp.logical_not(lends))
        def _():
            out_copy(i, e, 0, width).start()

        return carry

    relay(0)
    lax.fori_loop(0, 2 * heads, step, 0)

    if detour:
        @pl.when(chip == 0)
        def _():
            carry_on().wait_recv()
            hand_over().start()

    def leaving(core):
        return own.at[:, :, cols(core * heads * hd, heads * hd)]

    all_of(leaving(1 - p), send_sem.at[0]).wait_send()
    swap_q.wait_send()
    for core in range(2):
        for d in range(1, back + 1):
            go = chip + d < chips
            if detour and d == 1:
                go = go & (chip != 1)

            @pl.when(go)
            def _(core=core, d=d):
                all_of(leaving(core), send_sem.at[2 * d - 1 + core]).wait_send()
    if detour:
        @pl.when(chip == 1)
        def _():
            for core in range(2):
                all_of(piece(0), send_sem.at[1 + core]).wait_send()

        @pl.when(relays)
        def _():
            all_of(held.at[1:, :, 0:2], send_sem.at[1]).wait_send()
    if detour:
        @pl.when(chip == 0)
        def _():
            carry_on().wait_send()
            hand_over().wait_send()

    all_of(out_buf, out_send).wait_send()
    all_of(out_ref, out_recv).wait_recv()


def per_device(n, sections, queries, keys_new, values_new, stretch_cache, signs, docs):
    rows, q_width = queries.shape[1:]
    kv_width = keys_new.shape[-1]
    hd = signs.shape[-1]
    all_heads = kv_width // hd
    heads = all_heads // 2
    width = q_width // all_heads
    groups = width // hd
    reach = n // 2
    slots = reach + 2
    cached = stretch_cache.shape[1]
    dtype = queries.dtype
    dma = pltpu.SemaphoreType.DMA
    in_hbm = pl.BlockSpec(memory_space=pltpu.HBM)
    out = pl.pallas_call(
        functools.partial(attention_kernel, n, sections),
        out_shape=pltpu.VMEM((rows, q_width), dtype),
        in_specs=[in_hbm] * 6,
        out_specs=pl.BlockSpec(memory_space=pltpu.VMEM),
        scratch_shapes=[
            pltpu.SMEM(docs.shape, docs.dtype),
            pltpu.VMEM(signs.shape[1:], signs.dtype),
            pltpu.VMEM((2, rows, heads * width), dtype),
            pltpu.VMEM((rows, heads * width), dtype),
            pltpu.VMEM((2, cached, heads * hd), dtype),
            pltpu.VMEM((2, rows, kv_width), dtype),
            pltpu.VMEM((heads, 2, slots, rows, hd), dtype),
            pltpu.VMEM((heads, 2, rows, width), dtype),
            dma((2,)),
            dma,
            dma((2,)),
            dma,
            dma,
            dma,
            dma,
            dma((reach + 1,)),
            dma((heads, reach // 2 + 1)),
            dma,
            dma,
            pltpu.VMEM((2, rows, width // 2), dtype),
            dma((4,)),
        ],
        compiler_params=pltpu.CompilerParams(
            collective_id=0, has_side_effects=True, vmem_limit_bytes=58 * 1024 * 1024
        ),
    )(docs, signs[0], queries[0], keys_new[0], values_new[0], stretch_cache[0])
    return out[None]


def solution(mesh):
    in_specs = (
        P("section", "ctx", None),
        P("section", "ctx", None),
        P("section", "ctx", None),
        P("section", None, None),
        P("section", None, None),
        P(),
    )
    out_specs = P("section", "ctx", None)
    body = functools.partial(per_device, mesh.shape["ctx"], mesh.shape["section"])
    return jax.shard_map(body, mesh=mesh, in_specs=in_specs, out_specs=out_specs, check_vma=False)
```

```python
import functools

import jax
import jax.numpy as jnp
import numpy as np
from jax import lax
from jax.experimental import pallas as pl
from jax.experimental.pallas import tpu as pltpu
from jax.sharding import PartitionSpec as P

CACHE = 256
LENT = (4, 7)
PARTS = 3
MESH = pl.DeviceIdType.MESH


def attention_kernel(
    n,
    sections,
    docs_hbm,
    signs_hbm,
    q_hbm,
    k_hbm,
    v_hbm,
    cache_hbm,
    out_ref,
    docs_ref,
    signs_ref,
    q_buf,
    q_send,
    cache_buf,
    own,
    held,
    out_buf,
    small_sem,
    cache_sem,
    q_sem,
    swap_send,
    swap_recv,
    own_sem,
    mine_sem,
    send_sem,
    recv_sem,
    out_send,
    out_recv,
    pass_buf,
    pass_sem,
):
    section = lax.axis_index("section")
    me = lax.axis_index("ctx")
    p = lax.rem(me, 2)
    chip = me // 2
    chips = n // 2
    heads, hd = held.shape[0], held.shape[4]
    rows = held.shape[3]
    slots = held.shape[2]
    back = (slots - 2) // 2
    width = out_buf.shape[3]
    groups = width // hd
    all_heads = 2 * heads
    kv_width = all_heads * hd
    detour = chips == 4
    sibling = me + 1 - 2 * p
    following = lax.rem(section + 1, sections)
    previous = lax.rem(section + sections - 1, sections)

    def cols(start, size):
        return pl.ds(pl.multiple_of(start, hd), size)

    barrier = pltpu.get_barrier_semaphore()

    def greet(sec, ctx):
        pl.semaphore_signal(barrier, inc=1, device_id=(sec, ctx), device_id_type=MESH)

    own_copies = (
        pltpu.make_async_copy(k_hbm, own.at[0], own_sem),
        pltpu.make_async_copy(v_hbm, own.at[1], own_sem),
    )

    def mine_copies(i):
        at = cols((p * heads + i) * hd, hd)
        slot = slots - 2 + p
        return (
            pltpu.make_async_copy(k_hbm.at[:, at], held.at[i, 0, slot], mine_sem),
            pltpu.make_async_copy(v_hbm.at[:, at], held.at[i, 1, slot], mine_sem),
        )

    span = heads * width
    q_copies = (
        pltpu.make_async_copy(q_hbm.at[:, cols(p * span, span)], q_buf.at[p], q_sem.at[0]),
        pltpu.make_async_copy(q_hbm.at[:, cols((1 - p) * span, span)], q_send, q_sem.at[1]),
    )
    reach = heads * hd
    cache_copies = (
        pltpu.make_async_copy(
            cache_hbm.at[:, cols(p * reach, reach)], cache_buf.at[0], cache_sem
        ),
        pltpu.make_async_copy(
            cache_hbm.at[:, cols(kv_width + p * reach, reach)], cache_buf.at[1], cache_sem
        ),
    )
    small = (
        pltpu.make_async_copy(docs_hbm, docs_ref, small_sem.at[0]),
        pltpu.make_async_copy(signs_hbm, signs_ref, small_sem.at[1]),
    )
    def all_of(ref, sem):
        return pltpu.make_async_remote_copy(
            src_ref=ref,
            dst_ref=ref,
            send_sem=sem,
            recv_sem=sem,
            device_id=(section, sibling),
            device_id_type=MESH,
        )

    for copy in own_copies:
        copy.start()

    for d in range(back, 0, -1):
        come = chip >= d
        @pl.when(come)
        def _(d=d):
            greet(section, 2 * (chip - d))
            greet(section, 2 * (chip - d) + 1)
    if detour:
        @pl.when(chip == 2)
        def _():
            greet(section, me + 2)

        @pl.when(chip == 0)
        def _():
            greet(section, me + 4)
    greet(section, sibling)
    greet(previous, 2 * chip)
    greet(previous, 2 * chip + 1)

    for copy in small + mine_copies(0) + cache_copies + q_copies:
        copy.start()
    for i in range(1, heads):
        for copy in mine_copies(i):
            copy.start()

    for d in range(1, back + 1):
        @pl.when(chip < d)
        def _(d=d):
            for i in range(heads):
                at = slots - 2 - 2 * d
                held[i, :, at : at + 2] = jnp.zeros((2, 2, rows, hd), held.dtype)

    low = lax.broadcasted_iota(jnp.int32, (hd, hd), 0) & lax.broadcasted_iota(
        jnp.int32, (hd, hd), 1
    )
    shift = 1
    while 2 * shift < hd:
        shift *= 2
    while shift:
        low = low ^ (low >> shift)
        shift //= 2
    hada = (1 - 2 * (low & 1)).astype(jnp.float32).astype(jnp.bfloat16)

    count = jnp.int32(3)
    for d in range(1, back + 1):
        count = count + jnp.where(chip + d < chips, 2, 0)
    if detour:
        count = count + jnp.where(chip >= 2, 1, 0)
    pl.semaphore_wait(barrier, count)

    def remote(src, dst, index, i, pair, target):
        return pltpu.make_async_remote_copy(
            src_ref=src,
            dst_ref=dst,
            send_sem=send_sem.at[index],
            recv_sem=recv_sem.at[i, pair],
            device_id=(section, target),
            device_id_type=MESH,
        )

    swap_q = pltpu.make_async_remote_copy(
        src_ref=q_send,
        dst_ref=q_buf.at[p],
        send_sem=swap_send,
        recv_sem=swap_recv,
        device_id=(section, sibling),
        device_id_type=MESH,
    )

    def piece(h):
        return own.at[:, :, cols(h * hd, hd)]

    def swap_kv(i):
        block = piece((1 - p) * heads + i)
        return remote(block, held.at[i, :, slots - 2 + p], 0, i, back, sibling)

    def ahead(i, core):
        for d in range(1, back + 1):
            go = chip + d < chips
            if detour and d == 1:
                go = go & ((chip != 1) | (i == 0))

            @pl.when(go)
            def _(d=d):
                slot = slots - 2 - 2 * d + p
                block = piece(core * heads + i)
                target = 2 * (chip + d) + core
                remote(
                    block, held.at[i, :, slot], 2 * d - 1 + core, i, back - d, target
                ).start()

    def relay_copy(i):
        return remote(held.at[i, :, 0:2], held.at[i, :, 2:4], 1, i, 1, me - 2)

    def arrived(i, pair):
        block = held.at[i, :, 2 * pair : 2 * pair + 2]
        remote(block, block, 0, i, pair, sibling).wait_recv()

    relays = (chip == chips - 1) if detour else False

    def relay(i):
        if detour:
            @pl.when(relays)
            def _():
                arrived(i, 0)

                @pl.when(i > 0)
                def _():
                    relay_copy(i).start()

    def send(k, carry):
        i, core = k // 2, lax.rem(k, 2)
        if detour and heads % 2 == 0:
            pairs = chip == 1
            i = jnp.where(pairs, 2 * (k // 4) + lax.rem(k, 2), i)
            core = jnp.where(pairs, lax.rem(k // 2, 2), core)

        @pl.when(core == 0)
        def _():
            swap_kv(i).start()

        ahead(i, core)
        return carry

    all_of(own, own_sem).wait_recv()
    lax.fori_loop(0, 2 * heads, send, 0)
    q_copies[1].wait()
    swap_q.start()

    for copy in small:
        copy.wait()
    root = hd ** -0.5
    sign_k = signs_ref[0:1, :].astype(jnp.float32) * root
    sign_v = signs_ref[1:2, :].astype(jnp.float32) * root
    factor = root * float(np.log2(np.e))
    causal = lax.broadcasted_iota(jnp.int32, (rows, rows), 1) <= lax.broadcasted_iota(
        jnp.int32, (rows, rows), 0
    )

    def out_copy(i, e, start, size):
        return pltpu.make_async_remote_copy(
            src_ref=out_buf.at[i, e, :, start : start + size],
            dst_ref=out_ref.at[:, cols((p * heads + i) * width + start, size)],
            send_sem=out_send,
            recv_sem=out_recv,
            device_id=(following, 2 * chip + e),
            device_id_type=MESH,
        )

    def hop(src, dst, sem, recv, target):
        return pltpu.make_async_remote_copy(
            src_ref=src,
            dst_ref=dst,
            send_sem=sem,
            recv_sem=recv,
            device_id=target,
            device_id_type=MESH,
        )

    lent, held_back = LENT
    lender = (chip == 2) if detour else False
    lent_half = lent % 2
    lent_e = (p + lent_half) - 2 * p * lent_half
    share = pass_buf.shape[2]
    kept = width - share
    lent_out = out_ref.at[:, cols((p * heads + lent // 2) * width + kept, share)]

    def lend():
        return hop(
            out_buf.at[lent // 2, lent_e, :, kept:],
            pass_buf.at[0],
            out_send,
            pass_sem.at[0],
            (section, p),
        )

    def carry_on():
        return hop(
            pass_buf.at[0], pass_buf.at[1], pass_sem.at[1], pass_sem.at[2], (following, me)
        )

    def hand_over():
        return hop(pass_buf.at[1], lent_out, pass_sem.at[3], out_recv, (section, 4 + lent_e))

    def step(t, carry):
        i = t // 2
        half = lax.rem(t, 2)
        e = (p + half) - 2 * p * half
        lends = lender & (t == lent)
        in_parts = t == 1

        @pl.when(t == 0)
        def _():
            all_of(cache_buf, cache_sem).wait_recv()
            all_of(held.at[:, :, slots - 2 + p], mine_sem).wait_recv()
            q_copies[0].wait()

        stretch = 2 * chip + e
        doc = docs_ref[stretch]
        picks = [
            jnp.full((1, hd), jnp.where(doc == k, 1.0, 0.0), jnp.float32).astype(jnp.bfloat16)
            for k in range(cache_buf.shape[1] // CACHE)
        ]

        def cache_block(kind):
            terms = [
                cache_buf[kind, k * CACHE : (k + 1) * CACHE, cols(i * hd, hd)] * pick
                for k, pick in enumerate(picks)
            ]
            return functools.reduce(jnp.add, terms)

        back_k = jnp.dot(cache_block(0), hada, preferred_element_type=jnp.float32)
        back_v = jnp.dot(cache_block(1), hada, preferred_element_type=jnp.float32)
        back_k = (back_k * sign_k).astype(jnp.bfloat16)
        back_v = (back_v * sign_v).astype(jnp.bfloat16)
        biases = []
        for d in range(slots - 2, 0, -1):
            seen = (stretch >= d) & (docs_ref[jnp.maximum(stretch - d, 0)] == doc)
            biases.append(jnp.where(seen, 0.0, -jnp.inf).astype(jnp.float32))

        @pl.when(half == 0)
        def _():
            for pair in range(back):
                there = chip - back + pair >= 0
                if detour and pair == 0:
                    there = there & (chip != chips - 1)

                @pl.when(there)
                def _(pair=pair):
                    arrived(i, pair)

        @pl.when(half == 1 - p)
        def _():
            block = held.at[i, :, slots - 1 - p]
            remote(block, block, 0, i, back, sibling).wait_recv()

        @pl.when(t == 1)
        def _():
            swap_q.wait_recv()

        span_new = (slots - 1) * rows
        keys = held[i, 0, pl.ds(e, slots - 1)].reshape(span_new, hd)
        values = held[i, 1, pl.ds(e, slots - 1)].reshape(span_new, hd)
        keys = jnp.concatenate([back_k, keys], axis=0)
        values = jnp.concatenate([back_v, values], axis=0)
        for g in range(groups):
            query = q_buf[e, :, cols(i * width + g * hd, hd)]
            scores = lax.dot_general(
                query, keys, (((1,), (1,)), ((), ())), preferred_element_type=jnp.float32
            )
            parts = [scores[:, at : at + rows] for at in range(0, CACHE, rows)]
            for d in range(slots - 2):
                at = CACHE + rows * d
                parts.append(scores[:, at : at + rows] + biases[d])
            parts.append(jnp.where(causal, scores[:, CACHE + span_new - rows :], -jnp.inf))
            top = functools.reduce(jnp.maximum, parts)
            top = jnp.max(top, axis=1, keepdims=True)
            expo = [jnp.exp2((part - top) * factor) for part in parts]
            total = jnp.sum(functools.reduce(jnp.add, expo), axis=1, keepdims=True)
            weights = jnp.concatenate([part.astype(jnp.bfloat16) for part in expo], axis=1)
            summed = jnp.dot(weights, values, preferred_element_type=jnp.float32)
            out_buf[i, e, :, g * hd : (g + 1) * hd] = (summed / total).astype(out_buf.dtype)

            @pl.when((t == 0) | (t == 2))
            def _(g=g):
                out_copy(i, e, g * hd, hd).start()

            if g == groups // 2:
                @pl.when((half == 0) & (i + 1 < heads))
                def _():
                    relay(i + 1)

            if g == kept // hd - 1:
                @pl.when(lends)
                def _():
                    out_copy(i, e, 0, kept).start()

            if g == groups // 2 - 1:
                @pl.when(in_parts)
                def _():
                    out_copy(i, e, 0, width // 2).start()

        if detour:
            @pl.when((chip == 0) & (t == held_back))
            def _():
                lend().wait_recv()
                carry_on().start()

            @pl.when(lends)
            def _():
                lend().start()

        @pl.when(in_parts)
        def _():
            out_copy(i, e, width // 2, width // 2).start()

        @pl.when((t >= PARTS) & jnp.logical_not(lends))
        def _():
            out_copy(i, e, 0, width).start()

        return carry

    relay(0)
    lax.fori_loop(0, 2 * heads, step, 0)

    if detour:
        @pl.when(chip == 0)
        def _():
            carry_on().wait_recv()
            hand_over().start()

    def leaving(core):
        return own.at[:, :, cols(core * heads * hd, heads * hd)]

    all_of(leaving(1 - p), send_sem.at[0]).wait_send()
    swap_q.wait_send()
    for core in range(2):
        for d in range(1, back + 1):
            go = chip + d < chips
            if detour and d == 1:
                go = go & (chip != 1)

            @pl.when(go)
            def _(core=core, d=d):
                all_of(leaving(core), send_sem.at[2 * d - 1 + core]).wait_send()
    if detour:
        @pl.when(chip == 1)
        def _():
            for core in range(2):
                all_of(piece(0), send_sem.at[1 + core]).wait_send()

        @pl.when(relays)
        def _():
            all_of(held.at[1:, :, 0:2], send_sem.at[1]).wait_send()
    if detour:
        @pl.when(chip == 0)
        def _():
            carry_on().wait_send()
            hand_over().wait_send()

    all_of(out_buf, out_send).wait_send()
    all_of(out_ref, out_recv).wait_recv()


def per_device(n, sections, queries, keys_new, values_new, stretch_cache, signs, docs):
    rows, q_width = queries.shape[1:]
    kv_width = keys_new.shape[-1]
    hd = signs.shape[-1]
    all_heads = kv_width // hd
    heads = all_heads // 2
    width = q_width // all_heads
    groups = width // hd
    reach = n // 2
    slots = reach + 2
    cached = stretch_cache.shape[1]
    dtype = queries.dtype
    dma = pltpu.SemaphoreType.DMA
    in_hbm = pl.BlockSpec(memory_space=pltpu.HBM)
    out = pl.pallas_call(
        functools.partial(attention_kernel, n, sections),
        out_shape=pltpu.VMEM((rows, q_width), dtype),
        in_specs=[in_hbm] * 6,
        out_specs=pl.BlockSpec(memory_space=pltpu.VMEM),
        scratch_shapes=[
            pltpu.SMEM(docs.shape, docs.dtype),
            pltpu.VMEM(signs.shape[1:], signs.dtype),
            pltpu.VMEM((2, rows, heads * width), dtype),
            pltpu.VMEM((rows, heads * width), dtype),
            pltpu.VMEM((2, cached, heads * hd), dtype),
            pltpu.VMEM((2, rows, kv_width), dtype),
            pltpu.VMEM((heads, 2, slots, rows, hd), dtype),
            pltpu.VMEM((heads, 2, rows, width), dtype),
            dma((2,)),
            dma,
            dma((2,)),
            dma,
            dma,
            dma,
            dma,
            dma((reach + 1,)),
            dma((heads, reach // 2 + 1)),
            dma,
            dma,
            pltpu.VMEM((2, rows, width // 4 * 3), dtype),
            dma((4,)),
        ],
        compiler_params=pltpu.CompilerParams(
            collective_id=0, has_side_effects=True, vmem_limit_bytes=58 * 1024 * 1024
        ),
    )(docs, signs[0], queries[0], keys_new[0], values_new[0], stretch_cache[0])
    return out[None]


def solution(mesh):
    in_specs = (
        P("section", "ctx", None),
        P("section", "ctx", None),
        P("section", "ctx", None),
        P("section", None, None),
        P("section", None, None),
        P(),
    )
    out_specs = P("section", "ctx", None)
    body = functools.partial(per_device, mesh.shape["ctx"], mesh.shape["section"])
    return jax.shard_map(body, mesh=mesh, in_specs=in_specs, out_specs=out_specs, check_vma=False)
```
